32 devices in a mesh: grp: 2 (over x), pp: 4 (over z), dp: 4 (over y, core).
Axes of the slice: x: 2, y: 2, z: 4, core: 2. Of those that a mesh axis runs over, the one named last changes fastest.
Arguments:
- dy: bfloat16 [8, 256, 1024], P(('grp', 'pp'), 'dp'), parts along dimension 0
- xs: bfloat16 [8, 4, 1, 256, 1024], P(('grp', 'pp'), None, None, 'dp'), parts along dimension 0
- hs: bfloat16 [8, 4, 1, 256, 4096], P(('grp', 'pp'), None, None, 'dp'), parts along dimension 0
- w1: bfloat16 [8, 1, 1024, 4096], P(('grp', 'pp')), parts along dimension 0
- w2: bfloat16 [8, 1, 4096, 1024], P(('grp', 'pp')), parts along dimension 0
- acc1: float32 [8, 4, 1, 1024, 4096], P(('grp', 'pp'), 'dp'), parts along dimension 0
- acc2: float32 [8, 4, 1, 4096, 1024], P(('grp', 'pp'), 'dp'), parts along dimension 0
Outputs:
- output 1: float32 [8, 1, 1024, 4096], P(('grp', 'pp'), None, 'dp'), parts along dimension 0
- output 2: float32 [8, 1, 4096, 1024], P(('grp', 'pp'), None, 'dp'), parts along dimension 0
- output 3: bfloat16 [8, 256, 1024], P(('grp', 'pp'), 'dp'), parts along dimension 0
There are 2 independent parts. The reference program is written for one: setup_inputs(seed, part) draws one part's arguments, and reference() takes and returns one part's arrays. A program takes and returns all parts, laid end to end along the dimension named above; each array names one.
All inputs are finite; a program needn't handle non-finite values.
Results may differ from the reference program's by a relative error of at most 0.005103.
Values are sent between devices in bfloat16 or wider.
A program may use at most 1 GiB of HBM per device.

```python
import jax
import jax.numpy as jnp
from jax import lax

STAGES = 4
REPS = 4
LAYERS = 1
TOK = 64
DM = 1024
FF = 4096

TOKENS = TOK * REPS


def gelu_fn(v):
    return jax.nn.gelu(v, approximate=True)


def setup_inputs(seed: int = 0, part: int = 0) -> dict:
    key = jax.random.fold_in(jax.random.key(seed), part)
    ks = jax.random.split(key, 7)
    alpha = (2.0 * STAGES * LAYERS) ** -0.5
    s1 = 0.3 * alpha * (STAGES * TOK) ** 0.5
    s2 = 0.65 * (STAGES * TOK) ** 0.5
    dy = jax.random.normal(ks[0], (STAGES, TOKENS, DM), jnp.float32).astype(jnp.bfloat16)
    xs = jax.random.normal(ks[1], (STAGES, STAGES, LAYERS, TOKENS, DM), jnp.float32).astype(jnp.bfloat16)
    hs = jax.random.normal(ks[2], (STAGES, STAGES, LAYERS, TOKENS, FF), jnp.float32).astype(jnp.bfloat16)
    w1 = (jax.random.normal(ks[3], (STAGES, LAYERS, DM, FF), jnp.float32) * DM ** -0.5).astype(jnp.bfloat16)
    w2 = (jax.random.normal(ks[4], (STAGES, LAYERS, FF, DM), jnp.float32) * (FF ** -0.5 * alpha)).astype(jnp.bfloat16)
    acc1 = jax.random.normal(ks[5], (STAGES, REPS, LAYERS, DM, FF), jnp.float32) * s1
    acc2 = jax.random.normal(ks[6], (STAGES, REPS, LAYERS, FF, DM), jnp.float32) * s2
    return {'dy': dy, 'xs': xs, 'hs': hs, 'w1': w1, 'w2': w2, 'acc1': acc1, 'acc2': acc2}


def layer_back(g, x, h, wa, wb):
    act, act_vjp = jax.vjp(gelu_fn, h.astype(jnp.float32))
    u = jnp.dot(g, wb.T, preferred_element_type=jnp.float32)
    dh = act_vjp(u)[0].astype(jnp.bfloat16)
    gx = (g.astype(jnp.float32) + jnp.dot(dh, wa.T, preferred_element_type=jnp.float32)).astype(jnp.bfloat16)
    ab = act.astype(jnp.bfloat16)
    d1 = jnp.einsum('rtd,rtf->rdf', x.reshape(REPS, TOK, DM).astype(jnp.float32), dh.reshape(REPS, TOK, FF).astype(jnp.float32))
    d2 = jnp.einsum('rtf,rtd->rfd', ab.reshape(REPS, TOK, FF).astype(jnp.float32), g.reshape(REPS, TOK, DM).astype(jnp.float32))
    return gx, d1, d2


def stage_back(g, xk, hk, wa, wb, ga, gb):
    def body(c, inp):
        x, h, a1, a2, s1, s2 = inp
        gx, d1, d2 = layer_back(c, x, h, a1, a2)
        return gx, (s1 + d1, s2 + d2)
    gout, (ga2, gb2) = lax.scan(body, g, (xk, hk, wa, wb, ga, gb), reverse=True)
    return gout, ga2, gb2


def reference(dy, xs, hs, w1, w2, acc1, acc2):
    g1_rows = []
    g2_rows = []
    cots = []
    for s in reversed(range(STAGES)):
        ga = jnp.transpose(acc1[s], (1, 0, 2, 3))
        gb = jnp.transpose(acc2[s], (1, 0, 2, 3))
        incoming = cots + [dy[s]]
        outgoing = []
        for j in range(STAGES - s):
            gout, ga, gb = stage_back(incoming[j], xs[s, j], hs[s, j], w1[s], w2[s], ga, gb)
            outgoing.append(gout)
        cots = outgoing
        g1_rows.append(jnp.sum(ga.astype(jnp.bfloat16).astype(jnp.float32), axis=1) / REPS)
        g2_rows.append(jnp.sum(gb.astype(jnp.bfloat16).astype(jnp.float32), axis=1) / REPS)
    g1 = jnp.stack(g1_rows[::-1])
    g2 = jnp.stack(g2_rows[::-1])
    dx = jnp.stack(cots)
    return g1, g2, dx
```

```python
import functools

import jax
import jax.numpy as jnp
from jax import lax
from jax.experimental import pallas as pl
from jax.experimental.pallas import tpu as pltpu
from jax.sharding import PartitionSpec as P

MESH = pl.DeviceIdType.MESH
NN = (((1,), (0,)), ((), ()))
NT = (((1,), (1,)), ((), ()))
SQRT_2_OVER_PI = 0.7978845608028654
BF16 = jnp.bfloat16
F32 = jnp.float32


def dot(a, b, dims):
    return lax.dot_general(a, b, dims, preferred_element_type=F32)


def kernel(npp, ndp, tok, nchunk, dy, xs, hs, w1, w2, acc1, acc2, g1, g2, dx,
           w1v, w2v, recv1, recv2, hv, xv, act, slope, dht, xt, gall, gin, gout, dxin, ident,
           stage1, stage2, out1, out2,
           ld_sem, h_sem, w2_sem, w1_sem, st1_sem, st2_sem, o1_sem, o2_sem,
           hop_send, hop_recv, dx_recv, dx_sem, send1, recv1_sem, send2, recv2_sem):
    s = lax.axis_index('pp')
    p = lax.axis_index('dp')
    dm, ff = w1v.shape
    ntok = npp * tok
    blk = ident.shape[0]
    nw2 = 8
    w2rows = ff // nw2
    nblk = dm // blk
    q1 = dm // ndp
    q2 = ff // ndp
    c1 = ff // nchunk
    c2 = q2 // nchunk

    far = (p + 2) % ndp
    peer = (p, p + 1 - 2 * (p % 2), far, far + 1 - 2 * (far % 2))

    def w2_copy(i):
        rows = pl.ds(i * w2rows, w2rows)
        return pltpu.make_async_copy(w2.at[rows, :], w2v.at[rows, :], w2_sem.at[i])

    def w1_copy(i):
        rows = pl.ds(i * blk, blk)
        return pltpu.make_async_copy(w1.at[rows, :], w1v.at[rows, :], w1_sem.at[i])

    def acc1_copy(i, k):
        slot = i % 2
        src = acc1.at[pl.ds(peer[k] * q1, q1), pl.ds(pl.multiple_of(i * c1, c1), c1)]
        return pltpu.make_async_copy(src, stage1.at[slot, k], st1_sem.at[slot, k])

    def acc2_copy(i, k):
        slot = i % 2
        src = acc2.at[pl.ds(peer[k] * q2 + i * c2, c2), :]
        return pltpu.make_async_copy(src, stage2.at[slot, k], st2_sem.at[slot, k])

    def h_copy(j):
        rows = pl.ds(j * tok, tok)
        return pltpu.make_async_copy(hs.at[rows, :], hv.at[rows, :], h_sem.at[j])

    x_copy = pltpu.make_async_copy(xs, xv, ld_sem.at[0])
    for j in range(npp):
        @pl.when(j < npp - s)
        def _():
            h_copy(j).start()
    for c in range(nblk):
        pltpu.make_async_copy(dy.at[:, pl.ds(c * blk, blk)], gin.at[0, c], hop_recv.at[0, c]).start()
    for i in range(nw2):
        w2_copy(i).start()
    for i in range(nblk):
        w1_copy(i).start()
    x_copy.start()
    for i in range(2):
        for k in range(ndp):
            acc2_copy(i, k).start()
    for i in range(2):
        for k in range(ndp):
            acc1_copy(i, k).start()

    barrier = pltpu.get_barrier_semaphore()
    for k in range(1, ndp):
        pl.semaphore_signal(barrier, inc=1, device_id={'dp': peer[k]}, device_id_type=MESH)
    for k in range(1, npp):
        pl.semaphore_signal(barrier, inc=1, device_id={'pp': (s + k) % npp}, device_id_type=MESH)

    rid = lax.broadcasted_iota(jnp.int32, (blk, blk), 0)
    cid = lax.broadcasted_iota(jnp.int32, (blk, blk), 1)
    ident[...] = jnp.where(rid == cid, 1.0, 0.0).astype(BF16)
    gall[...] = jnp.zeros_like(gall)

    for j in range(npp):
        @pl.when(j < npp - s)
        def _():
            h_copy(j).wait()

        @pl.when(j >= npp - s)
        def _():
            hv[j * tok:(j + 1) * tok, :] = jnp.zeros((tok, ff), BF16)

    def gelu_step(i, _):
        rows = pl.ds(pl.multiple_of(i * blk, blk), blk)
        h = dot(ident[...], hv[:, rows], NT)
        t = jnp.tanh(SQRT_2_OVER_PI * (h + 0.044715 * (h * h * h)))
        cdf = 0.5 * (1.0 + t)
        act[rows, :] = (h * cdf).astype(BF16)
        inner = SQRT_2_OVER_PI * (1.0 + (3.0 * 0.044715) * (h * h))
        slope[rows, :] = cdf + 0.5 * h * ((1.0 + t) * (1.0 - t)) * inner
        return 0

    lax.fori_loop(0, ff // blk, gelu_step, 0)

    pl.semaphore_wait(barrier, ndp - 1 + npp - 1)

    def hop_copy(t, c, to):
        return pltpu.make_async_remote_copy(
            src_ref=gout.at[t, c], dst_ref=gin.at[t + 1, c], send_sem=hop_send.at[t, c], recv_sem=hop_recv.at[t + 1, c],
            device_id={'pp': to}, device_id_type=MESH)

    def dx_copy(t, c, to):
        return pltpu.make_async_remote_copy(
            src_ref=gout.at[t, c], dst_ref=dxin.at[c], send_sem=hop_send.at[t, c], recv_sem=dx_recv.at[c],
            device_id={'pp': to}, device_id_type=MESH)

    for t in range(npp):
        j = npp - 1 - t - s

        @pl.when(j >= 0)
        def _(t=t, j=j):
            trows = pl.ds(pl.multiple_of(j * tok, tok), tok)
            for c in range(nblk):
                if t == 0:
                    pltpu.make_async_copy(dy.at[:, pl.ds(c * blk, blk)], gin.at[0, c], hop_recv.at[0, c]).wait()
                else:
                    hop_copy(t - 1, c, s).wait_recv()
                gall[trows, c * blk:(c + 1) * blk] = gin[t, c]

            def u_step(i, _):
                if t == 0:
                    w2_copy(i).wait()
                rows = pl.ds(pl.multiple_of(i * w2rows, w2rows), w2rows)
                u = dot(w2v[rows, :], gall[...], NT)
                dht[rows, :] = (slope[rows, :] * u).astype(BF16)
                return 0

            lax.fori_loop(0, nw2, u_step, 0)

            def gx_step(c, _):
                if t == 0:
                    w1_copy(c).wait()
                rows = pl.ds(pl.multiple_of(c * blk, blk), blk)
                z = dot(ident[...], gall[:, rows], NT) + dot(w1v[rows, :], dht[...], NN)
                zt = dot(ident[trows, :], z.astype(BF16), NT)
                gout[t, c] = zt.astype(BF16)

                if t < npp - 1:
                    @pl.when(s > 0)
                    def _():
                        hop_copy(t, c, jnp.maximum(s - 1, 0)).start()

                    @pl.when(s == 0)
                    def _():
                        dx_copy(t, c, npp - 1 - t).start()
                return 0

            lax.fori_loop(0, nblk, gx_step, 0)

    x_copy.wait()
    for c in range(nblk):
        rows = pl.ds(c * blk, blk)
        xt[rows, :] = dot(ident[...], xv[:, rows], NT).astype(BF16)

    def send2_copy(i, k):
        return pltpu.make_async_remote_copy(
            src_ref=w2v.at[pl.ds(peer[k] * q2 + i * c2, c2), :], dst_ref=recv2.at[k - 1, i],
            send_sem=send2.at[k - 1, i], recv_sem=recv2_sem.at[k - 1, i], device_id={'dp': peer[k]}, device_id_type=MESH)

    def send1_copy(i, k):
        return pltpu.make_async_remote_copy(
            src_ref=w1v.at[pl.ds(peer[k] * q1, q1), pl.ds(pl.multiple_of(i * c1, c1), c1)], dst_ref=recv1.at[k - 1, i],
            send_sem=send1.at[k - 1, i], recv_sem=recv1_sem.at[k - 1, i], device_id={'dp': peer[k]}, device_id_type=MESH)

    order = (2, 3, 1, 0)

    def a2_step(i, _):
        slot = i % 2
        for k in order:
            acc2_copy(i, k).wait()
            rows = pl.ds(pl.multiple_of(peer[k] * q2 + i * c2, c2), c2)
            w2v[rows, :] = (stage2[slot, k] + dot(act[rows, :], gall[...], NN)).astype(BF16)
        for k in order[:-1]:
            send2_copy(i, k).start()

        @pl.when(i + 2 < nchunk)
        def _():
            for k in range(ndp):
                acc2_copy(i + 2, k).start()
        return 0

    lax.fori_loop(0, nchunk, a2_step, 0)

    def a1_step(i, _):
        slot = i % 2
        cols = pl.ds(pl.multiple_of(i * c1, c1), c1)
        for k in order:
            acc1_copy(i, k).wait()
            rows = pl.ds(pl.multiple_of(peer[k] * q1, q1), q1)
            w1v[rows, cols] = (stage1[slot, k] + dot(xt[rows, :], dht[cols, :], NT)).astype(BF16)
        for k in order[:-1]:
            send1_copy(i, k).start()

        @pl.when(i + 2 < nchunk)
        def _():
            for k in range(ndp):
                acc1_copy(i + 2, k).start()
        return 0

    lax.fori_loop(0, nchunk, a1_step, 0)

    for c in range(nblk):
        out = dx.at[:, pl.ds(c * blk, blk)]

        @pl.when(s == 0)
        def _():
            pltpu.make_async_copy(gout.at[npp - 1, c], out, dx_sem.at[c]).start()

        @pl.when(s > 0)
        def _():
            dx_copy(0, c, 0).wait_recv()
            pltpu.make_async_copy(dxin.at[c], out, dx_sem.at[c]).start()

    def out2_copy(i):
        return pltpu.make_async_copy(out2.at[i % 2], g2.at[pl.ds(i * c2, c2), :], o2_sem.at[i % 2])

    def out1_copy(i):
        return pltpu.make_async_copy(out1.at[i % 2], g1.at[:, pl.ds(pl.multiple_of(i * c1, c1), c1)], o1_sem.at[i % 2])

    scale = 1.0 / ndp

    def r2_step(i, _):
        @pl.when(i >= 2)
        def _():
            out2_copy(i - 2).wait()
        rows = pl.ds(pl.multiple_of(p * q2 + i * c2, c2), c2)
        tot = w2v[rows, :].astype(F32)
        for k in order[:-1]:
            send2_copy(i, k).wait()
        for k in range(1, ndp):
            tot = tot + recv2[k - 1, i].astype(F32)
        out2[i % 2] = tot * scale
        out2_copy(i).start()
        return 0

    lax.fori_loop(0, nchunk, r2_step, 0)

    def r1_step(i, _):
        @pl.when(i >= 2)
        def _():
            out1_copy(i - 2).wait()
        rows = pl.ds(pl.multiple_of(p * q1, q1), q1)
        cols = pl.ds(pl.multiple_of(i * c1, c1), c1)
        tot = w1v[rows, cols].astype(F32)
        for k in order[:-1]:
            send1_copy(i, k).wait()
        for k in range(1, ndp):
            tot = tot + recv1[k - 1, i].astype(F32)
        out1[i % 2] = tot * scale
        out1_copy(i).start()
        return 0

    lax.fori_loop(0, nchunk, r1_step, 0)

    for i in range(nchunk - 2, nchunk):
        out2_copy(i).wait()
        out1_copy(i).wait()
    for c in range(nblk):
        pltpu.make_async_copy(dxin.at[c], dx.at[:, pl.ds(c * blk, blk)], dx_sem.at[c]).wait()
    for t in range(npp):
        for c in range(nblk):
            if t < npp - 1:
                @pl.when(npp - 1 - t - s >= 0)
                def _():
                    hop_copy(t, c, 0).wait_send()


def solution(mesh):
    npp = mesh.shape['pp']
    ndp = mesh.shape['dp']

    def body(dy, xs, hs, w1, w2, acc1, acc2):
        tok = dy.shape[1]
        dm, ff = w1.shape[2:]
        ntok = npp * tok
        nchunk = 8
        blk = 256
        nblk = dm // blk
        q1, q2 = dm // ndp, ff // ndp
        c1, c2 = ff // nchunk, q2 // nchunk
        dma = pltpu.SemaphoreType.DMA
        any_spec = pl.BlockSpec(memory_space=pl.ANY)
        r1, r2, dx = pl.pallas_call(
            functools.partial(kernel, npp, ndp, tok, nchunk),
            out_shape=(jax.ShapeDtypeStruct((q1, ff), F32), jax.ShapeDtypeStruct((q2, dm), F32),
                       jax.ShapeDtypeStruct((tok, dm), BF16)),
            in_specs=[any_spec] * 7,
            out_specs=(any_spec,) * 3,
            scratch_shapes=[
                pltpu.VMEM((dm, ff), BF16), pltpu.VMEM((ff, dm), BF16),
                pltpu.VMEM((ndp - 1, nchunk, q1, c1), BF16), pltpu.VMEM((ndp - 1, nchunk, c2, dm), BF16),
                pltpu.VMEM((ntok, ff), BF16), pltpu.VMEM((ntok, dm), BF16),
                pltpu.VMEM((ff, ntok), BF16), pltpu.VMEM((ff, ntok), F32), pltpu.VMEM((ff, ntok), BF16),
                pltpu.VMEM((dm, ntok), BF16), pltpu.VMEM((ntok, dm), BF16),
                pltpu.VMEM((npp, nblk, tok, blk), BF16), pltpu.VMEM((npp, nblk, tok, blk), BF16),
                pltpu.VMEM((nblk, tok, blk), BF16), pltpu.VMEM((blk, blk), BF16),
                pltpu.VMEM((2, ndp, q1, c1), F32), pltpu.VMEM((2, ndp, c2, dm), F32),
                pltpu.VMEM((2, q1, c1), F32), pltpu.VMEM((2, c2, dm), F32),
                dma((1,)), dma((npp,)), dma((8,)), dma((nblk,)), dma((2, ndp)), dma((2, ndp)), dma((2,)), dma((2,)),
                dma((npp, nblk)), dma((npp, nblk)), dma((nblk,)), dma((nblk,)),
                dma((ndp - 1, nchunk)), dma((ndp - 1, nchunk)), dma((ndp - 1, nchunk)), dma((ndp - 1, nchunk)),
            ],
            compiler_params=pltpu.CompilerParams(
                collective_id=0, has_side_effects=True, vmem_limit_bytes=62 * 1024 * 1024),
        )(dy[0], xs.reshape(ntok, dm), hs.reshape(ntok, ff), w1[0, 0], w2[0, 0], acc1[0, 0, 0], acc2[0, 0, 0])
        return r1[None, None], r2[None, None], dx[None]

    spec_row = P(('grp', 'pp'), 'dp', None)
    spec_saved = P(('grp', 'pp'), None, None, 'dp', None)
    spec_w = P(('grp', 'pp'), None, None, None)
    spec_acc = P(('grp', 'pp'), 'dp', None, None, None)
    spec_g = P(('grp', 'pp'), None, 'dp', None)
    return jax.shard_map(body, mesh=mesh, in_specs=(spec_row, spec_saved, spec_saved, spec_w, spec_w, spec_acc, spec_acc), out_specs=(spec_g, spec_g, spec_row), check_vma=False)
```

```python
import functools

import jax
import jax.numpy as jnp
from jax import lax
from jax.experimental import pallas as pl
from jax.experimental.pallas import tpu as pltpu
from jax.sharding import PartitionSpec as P

MESH = pl.DeviceIdType.MESH
NN = (((1,), (0,)), ((), ()))
NT = (((1,), (1,)), ((), ()))
SQRT_2_OVER_PI = 0.7978845608028654
BF16 = jnp.bfloat16
F32 = jnp.float32


def dot(a, b, dims):
    return lax.dot_general(a, b, dims, preferred_element_type=F32)


def kernel(npp, ndp, tok, nchunk, dy, xs, hs, w1, w2, acc1, acc2, g1, g2, dx,
           w1v, w2v, recv1, recv2, hv, xv, act, slope, dht, xt, gt, uacc, first, gin, gout, dxin, ident,
           stage, dyv,
           ld_sem, h_sem, x_sem, w2_sem, w1_sem, st_sem,
           hop_send, hop_recv, dx_recv, send1, recv1_sem, send2, recv2_sem):
    s = lax.axis_index('pp')
    p = lax.axis_index('dp')
    dm, ff = w1v.shape
    blk = ident.shape[0]
    half = 2 * tok
    hb = blk // 2
    nw2 = w2_sem.shape[0]
    w2rows = ff // nw2
    nblk = dm // blk
    q1 = dm // ndp
    q2 = ff // ndp
    rc, cc = first.shape[1:]
    halves = q1 // rc
    mrows = 1024

    far = (p + 2) % ndp
    peer = (p, p + 1 - 2 * (p % 2), far, far + 1 - 2 * (far % 2))

    def w2_copy(i):
        rows = pl.ds(i * w2rows, w2rows)
        return pltpu.make_async_copy(w2.at[rows, :], w2v.at[rows, :], w2_sem.at[i])

    def w1_copy(i):
        rows = pl.ds(i * blk, blk)
        return pltpu.make_async_copy(w1.at[rows, :], w1v.at[rows, :], w1_sem.at[i])

    def rows1(i, k):
        return pl.ds(pl.multiple_of(peer[k] * q1 + (i % halves) * rc, rc), rc)

    def cols1(i):
        return pl.ds(pl.multiple_of((i // halves) * cc, cc), cc)

    def rows2(i, k):
        return pl.ds(pl.multiple_of(peer[k] * q2 + i * rc, rc), rc)

    def acc1_copy(i, k):
        slot = i % 2
        return pltpu.make_async_copy(acc1.at[rows1(i, k), cols1(i)], stage.at[slot, k], st_sem.at[slot, k])

    def acc2_copy(i, k):
        slot = i % 2
        return pltpu.make_async_copy(acc2.at[rows2(i, k), :], stage.at[slot, k], st_sem.at[slot, k])

    def h_copy(t):
        rows = pl.ds((npp - 1 - s - t) * tok, tok)
        return pltpu.make_async_copy(hs.at[rows, :], hv.at[pl.ds(t * tok, tok), :], h_sem.at[t])

    def x_copy(t):
        rows = pl.ds((npp - 1 - s - t) * tok, tok)
        return pltpu.make_async_copy(xs.at[rows, :], xv.at[pl.ds(t * tok, tok), :], x_sem.at[t])

    dy_copy = pltpu.make_async_copy(dy, dyv, ld_sem.at[0])

    def used(t, start):
        @pl.when(t < npp - s)
        def _():
            start(t)

    for t in range(2):
        used(t, lambda t: h_copy(t).start())
    dy_copy.start()

    barrier = pltpu.get_barrier_semaphore()
    for k in range(1, ndp):
        pl.semaphore_signal(barrier, inc=1, device_id={'dp': peer[k]}, device_id_type=MESH)
    for k in range(1, npp):
        pl.semaphore_signal(barrier, inc=1, device_id={'pp': (s + k) % npp}, device_id_type=MESH)

    rid = lax.broadcasted_iota(jnp.int32, (blk, blk), 0)
    cid = lax.broadcasted_iota(jnp.int32, (blk, blk), 1)
    ident[...] = jnp.where(rid == cid, 1.0, 0.0).astype(BF16)
    low = lax.broadcasted_iota(jnp.int32, (hb, half), 1) < tok

    def h_wait(t):
        @pl.when(t < npp - s)
        def _():
            h_copy(t).wait()

        @pl.when(t >= npp - s)
        def _():
            hv[t * tok:(t + 1) * tok, :] = jnp.zeros((tok, ff), BF16)

    def gelu_block(i, lanes):
        rows = pl.ds(pl.multiple_of(i * blk, blk), blk)
        h = dot(ident[...], hv[lanes, rows], NT)
        h2 = h * h
        t = jnp.tanh(SQRT_2_OVER_PI * (h + 0.044715 * (h2 * h)))
        cdf = 0.5 * (1.0 + t)
        act[rows, lanes] = (h * cdf).astype(BF16)
        inner = SQRT_2_OVER_PI * (1.0 + (3.0 * 0.044715) * h2)
        slope[rows, lanes] = cdf + 0.5 * h * ((1.0 + t) * (1.0 - t)) * inner

    def gelu(hh):
        def step(i, _):
            gelu_block(i, slice(hh * half, (hh + 1) * half))
            return 0

        with jax.named_scope('gelu'):
            lax.fori_loop(0, ff // blk, step, 0, unroll=4)

    with jax.named_scope('hwait'):
        for t in range(2):
            h_wait(t)
        dy_copy.wait()
    for i in range(nw2):
        w2_copy(i).start()
    gt[...] = jnp.zeros_like(gt)
    for c in range(nblk):
        gt[c * blk:(c + 1) * blk, 0:tok] = dot(ident[...], dyv[:, c * blk:(c + 1) * blk], NT).astype(BF16)
    for i in range(nblk):
        w1_copy(i).start()
    for t in range(2, npp):
        used(t, lambda t: h_copy(t).start())
    for t in range(npp):
        used(t, lambda t: x_copy(t).start())

    def hop_copy(t, c, to):
        return pltpu.make_async_remote_copy(
            src_ref=gout.at[t, c], dst_ref=gin.at[t, c], send_sem=hop_send.at[t, c], recv_sem=hop_recv.at[t, c],
            device_id={'pp': to}, device_id_type=MESH)

    def dx_copy(t, c, to):
        return pltpu.make_async_remote_copy(
            src_ref=gout.at[t, c], dst_ref=dxin.at[c], send_sem=hop_send.at[t, c], recv_sem=dx_recv.at[c],
            device_id={'pp': to}, device_id_type=MESH)

    def send_first(k):
        return pltpu.make_async_remote_copy(
            src_ref=first.at[k], dst_ref=recv2.at[k - 1, 0], send_sem=send2.at[k - 1, 0], recv_sem=recv2_sem.at[k - 1, 0],
            device_id={'dp': peer[k]}, device_id_type=MESH)

    order = (2, 3, 1, 0)

    def first_chunk():
        with jax.named_scope('first'):
            for k in order:
                acc2_copy(0, k).wait()
                rows = rows2(0, k)
                first[k] = (stage[0, k] + dot(act[rows, :], gt[...], NT)).astype(BF16)
                if k == order[1]:
                    send_first(order[0]).start()
                    send_first(order[1]).start()
            send_first(order[2]).start()
            for k in range(ndp):
                acc2_copy(2, k).start()

    def unpack(packed, c, t):
        lanes = slice((t // 2) * half, (t // 2 + 1) * half)
        v = packed.astype(F32)
        r = pltpu.roll(v, tok, 1)
        for b, (lo, hi) in enumerate(((v, r), (r, v))):
            rows = slice(c * blk + b * hb, c * blk + (b + 1) * hb)
            if t % 2 == 0:
                new = jnp.where(low, lo, 0.0)
            else:
                new = jnp.where(low, gt[rows, lanes].astype(F32), hi)
            gt[rows, lanes] = new.astype(BF16)

    for t in range(npp):
        lanes = slice((t // 2) * half, (t // 2 + 1) * half)

        @pl.when(t < npp - s)
        def _(t=t, lanes=lanes):
            if t == 0:
                def u_step(i, _):
                    w2_copy(i).wait()
                    for b in range(w2rows // blk):
                        gelu_block(i * (w2rows // blk) + b, lanes)
                    rows = pl.ds(pl.multiple_of(i * w2rows, w2rows), w2rows)
                    u = dot(w2v[rows, :], gt[:, lanes], NN)
                    dht[rows, lanes] = (slope[rows, lanes] * u).astype(BF16)
                    return 0

                with jax.named_scope('u0'):
                    lax.fori_loop(0, nw2, u_step, 0)
                with jax.named_scope('barrier'):
                    pl.semaphore_wait(barrier, ndp - 1 + npp - 1)
            else:
                for c in range(nblk):
                    with jax.named_scope('gwait'):
                        hop_copy(t - 1, c, s).wait_recv()
                    unpack(gin[t - 1, c], c, t)
                    if t == npp - 1 and c == nblk - 1:
                        first_chunk()
                    krows = slice(c * blk, (c + 1) * blk)

                    def u_step(i, _):
                        rows = pl.ds(pl.multiple_of(i * mrows, mrows), mrows)
                        u = dot(w2v[rows, krows], gt[krows, lanes], NN)
                        if c > 0:
                            u = uacc[rows, :] + u
                        if c < nblk - 1:
                            uacc[rows, :] = u
                        else:
                            dht[rows, lanes] = (slope[rows, lanes] * u).astype(BF16)
                        return 0

                    with jax.named_scope('u'):
                        lax.fori_loop(0, ff // mrows, u_step, 0, unroll=True)

            def gx_dot(c):
                if t == 0:
                    w1_copy(c).wait()
                rows = slice(c * blk, (c + 1) * blk)
                return gt[rows, lanes].astype(F32) + dot(w1v[rows, :], dht[:, lanes], NN)

            def gx_put(c, z):
                top, bot = z[:hb], z[hb:]
                if t % 2 == 0:
                    z = jnp.where(low, top, pltpu.roll(bot, tok, 1))
                else:
                    z = jnp.where(low, pltpu.roll(top, tok, 1), bot)
                gout[t, c] = z.astype(BF16)

                if t < npp - 1:
                    @pl.when(s > 0)
                    def _():
                        hop_copy(t, c, jnp.maximum(s - 1, 0)).start()

                    @pl.when(s == 0)
                    def _():
                        dx_copy(t, c, npp - 1 - t).start()

            with jax.named_scope('gx'):
                z = gx_dot(0)
                for c in range(1, nblk):
                    z, last = gx_dot(c), z
                    gx_put(c - 1, last)
                gx_put(nblk - 1, z)

        if t == 0:
            for i in range(2):
                for k in range(ndp):
                    acc2_copy(i, k).start()
            @pl.when(s < npp - 2)
            def _():
                for t in range(2, npp):
                    h_wait(t)
                gelu(1)

            @pl.when(s >= npp - 2)
            def _():
                act[:, half:] = jnp.zeros((ff, half), BF16)
                dht[:, half:] = jnp.zeros((ff, half), BF16)

    @pl.when(s > 0)
    def _():
        first_chunk()

    for t in range(npp):
        @pl.when(t < npp - s)
        def _():
            x_copy(t).wait()

        @pl.when(t >= npp - s)
        def _():
            xv[t * tok:(t + 1) * tok, :] = jnp.zeros((tok, dm), BF16)
    for c in range(nblk):
        rows = pl.ds(c * blk, blk)
        xt[rows, :] = dot(ident[...], xv[:, rows], NT).astype(BF16)

    def send2_copy(i, k):
        return pltpu.make_async_remote_copy(
            src_ref=w2v.at[rows2(i, k), :], dst_ref=recv2.at[k - 1, i],
            send_sem=send2.at[k - 1, i], recv_sem=recv2_sem.at[k - 1, i], device_id={'dp': peer[k]}, device_id_type=MESH)

    def send1_copy(i, k):
        return pltpu.make_async_remote_copy(
            src_ref=w1v.at[rows1(i, k), cols1(i)], dst_ref=recv1.at[k - 1, i],
            send_sem=send1.at[k - 1, i], recv_sem=recv1_sem.at[k - 1, i], device_id={'dp': peer[k]}, device_id_type=MESH)

    def a2_step(i, _):
        slot = i % 2
        for k in order:
            acc2_copy(i, k).wait()
            rows = rows2(i, k)
            w2v[rows, :] = (stage[slot, k] + dot(act[rows, :], gt[...], NT)).astype(BF16)
        for k in order[:-1]:
            send2_copy(i, k).start()

        @pl.when(i + 2 < nchunk)
        def _():
            for k in range(ndp):
                acc2_copy(i + 2, k).start()

        @pl.when(i + 2 >= nchunk)
        def _():
            for k in range(ndp):
                acc1_copy(i + 2 - nchunk, k).start()
        return 0

    with jax.named_scope('a2'):
        lax.fori_loop(1, nchunk, a2_step, 0)

    def a1_step(i, _):
        slot = i % 2
        for k in order:
            acc1_copy(i, k).wait()
            w1v[rows1(i, k), cols1(i)] = (
                stage[slot, k] + dot(xt[rows1(i, k), :], dht[cols1(i), :], NT)).astype(BF16)
        for k in order[:-1]:
            send1_copy(i, k).start()

        @pl.when(i + 2 < nchunk)
        def _():
            for k in range(ndp):
                acc1_copy(i + 2, k).start()
        return 0

    with jax.named_scope('a1'):
        lax.fori_loop(0, nchunk, a1_step, 0)

    def put_dx(packed, c, e):
        v = packed.astype(F32)
        r = pltpu.roll(v, tok, 1)
        col = jnp.concatenate([v, r], axis=0).astype(BF16)
        dx[:, c * blk:(c + 1) * blk] = dot(ident[:tok, :half], col, NT).astype(BF16)

    for c in range(nblk):
        @pl.when(s == 0)
        def _():
            put_dx(gout[npp - 1, c], c, 0)

        @pl.when(s > 0)
        def _():
            dx_copy(0, c, 0).wait_recv()
            put_dx(dxin[c], c, 0)

    scale = 1.0 / ndp

    def r2_sum(i, own):
        for k in range(1, ndp):
            own = own + recv2[k - 1, i].astype(F32)
        g2[pl.ds(pl.multiple_of(i * rc, rc), rc), :] = own * scale

    for k in order[:-1]:
        send_first(k).wait()
    r2_sum(0, first[0].astype(F32))

    def r2_step(i, _):
        with jax.named_scope('r2wait'):
            for k in order[:-1]:
                send2_copy(i, k).wait()
        r2_sum(i, w2v[rows2(i, 0), :].astype(F32))
        return 0

    lax.fori_loop(1, nchunk, r2_step, 0)

    def r1_step(i, _):
        with jax.named_scope('r1wait'):
            for k in order[:-1]:
                send1_copy(i, k).wait()
        tot = w1v[rows1(i, 0), cols1(i)].astype(F32)
        for k in range(1, ndp):
            tot = tot + recv1[k - 1, i].astype(F32)
        g1[pl.ds(pl.multiple_of((i % halves) * rc, rc), rc), cols1(i)] = tot * scale
        return 0

    lax.fori_loop(0, nchunk, r1_step, 0)

    for t in range(npp - 1):
        @pl.when(t < npp - s)
        def _():
            for c in range(nblk):
                hop_copy(t, c, 0).wait_send()


def solution(mesh):
    npp = mesh.shape['pp']
    ndp = mesh.shape['dp']

    def body(dy, xs, hs, w1, w2, acc1, acc2):
        tok = dy.shape[1]
        dm, ff = w1.shape[2:]
        ntok = npp * tok
        nchunk = 8
        blk = 256
        nblk = dm // blk
        q1, q2 = dm // ndp, ff // ndp
        rc, cc = q2 // nchunk, dm
        dma = pltpu.SemaphoreType.DMA
        any_spec = pl.BlockSpec(memory_space=pl.ANY)
        vmem = pl.BlockSpec(memory_space=pltpu.VMEM)
        shapes = ((q1, ff), F32), ((q2, dm), F32), ((tok, dm), BF16)
        outs = pl.pallas_call(
            functools.partial(kernel, npp, ndp, tok, nchunk),
            out_shape=tuple(pltpu.VMEM(shape, dtype) for shape, dtype in shapes),
            in_specs=[any_spec] * 7,
            out_specs=(vmem,) * 3,
            scratch_shapes=[
                pltpu.VMEM((dm, ff), BF16), pltpu.VMEM((ff, dm), BF16),
                pltpu.VMEM((ndp - 1, nchunk, rc, cc), BF16), pltpu.VMEM((ndp - 1, nchunk, rc, cc), BF16),
                pltpu.VMEM((ntok, ff), BF16), pltpu.VMEM((ntok, dm), BF16),
                pltpu.VMEM((ff, ntok), BF16), pltpu.VMEM((ff, ntok), F32), pltpu.VMEM((ff, ntok), BF16),
                pltpu.VMEM((dm, ntok), BF16), pltpu.VMEM((dm, ntok), BF16), pltpu.VMEM((ff, 2 * tok), F32),
                pltpu.VMEM((ndp, rc, cc), BF16),
                pltpu.VMEM((npp - 1, nblk, blk // 2, 2 * tok), BF16), pltpu.VMEM((npp, nblk, blk // 2, 2 * tok), BF16),
                pltpu.VMEM((nblk, blk // 2, 2 * tok), BF16), pltpu.VMEM((blk, blk), BF16),
                pltpu.VMEM((2, ndp, rc, cc), F32), pltpu.VMEM((tok, dm), BF16),
                dma((1,)), dma((npp,)), dma((npp,)), dma((8,)), dma((nblk,)), dma((2, ndp)),
                dma((npp - 1, nblk)), dma((npp - 1, nblk)), dma((nblk,)),
                dma((ndp - 1, nchunk)), dma((ndp - 1, nchunk)), dma((ndp - 1, nchunk)), dma((ndp - 1, nchunk)),
            ],
            compiler_params=pltpu.CompilerParams(
                collective_id=0, has_side_effects=True, vmem_limit_bytes=52 * 1024 * 1024),
        )(dy[0], xs.reshape(ntok, dm), hs.reshape(ntok, ff), w1[0, 0], w2[0, 0], acc1[0, 0, 0], acc2[0, 0, 0])
        r1, r2, dx = outs
        return r1[None, None], r2[None, None], dx[None]

    spec_row = P(('grp', 'pp'), 'dp', None)
    spec_saved = P(('grp', 'pp'), None, None, 'dp', None)
    spec_w = P(('grp', 'pp'), None, None, None)
    spec_acc = P(('grp', 'pp'), 'dp', None, None, None)
    spec_g = P(('grp', 'pp'), None, 'dp', None)
    return jax.shard_map(body, mesh=mesh, in_specs=(spec_row, spec_saved, spec_saved, spec_w, spec_w, spec_acc, spec_acc), out_specs=(spec_g, spec_g, spec_row), check_vma=False)
```

```python
import functools

import jax
import jax.numpy as jnp
from jax import lax
from jax.experimental import pallas as pl
from jax.experimental.pallas import tpu as pltpu
from jax.sharding import PartitionSpec as P

MESH = pl.DeviceIdType.MESH
NN = (((1,), (0,)), ((), ()))
NT = (((1,), (1,)), ((), ()))
SQRT_2_OVER_PI = 0.7978845608028654
BF16 = jnp.bfloat16
F32 = jnp.float32


def dot(a, b, dims):
    return lax.dot_general(a, b, dims, preferred_element_type=F32)


def kernel(npp, ndp, tok, nchunk, dy, xs, hs, w1, w2, acc1, acc2, g1, g2, dx,
           w1v, w2v, recv1, recv2, hv, xv, act, slope, dht, xt, gt, uacc, first, gin, gout, relay, ident,
           stage, dyv,
           ld_sem, h_sem, x_sem, w2_sem, w1_sem, st_sem,
           hop_send, hop_recv, send1, recv1_sem, send2, recv2_sem, unit_send, unit_recv, relay_send, relay_recv):
    s = lax.axis_index('pp')
    p = lax.axis_index('dp')
    dm, ff = w1v.shape
    blk = ident.shape[0]
    half = 2 * tok
    hb = blk // 2
    nw2 = w2_sem.shape[0]
    w2rows = ff // nw2
    nblk = dm // blk
    q1 = dm // ndp
    q2 = ff // ndp
    rc, cc = first.shape[1:]
    halves = q1 // rc
    mrows = 1024
    ru = rc // 2
    shed = (3, 1)

    far = (p + 2) % ndp
    peer = (p, p + 1 - 2 * (p % 2), far, far + 1 - 2 * (far % 2))

    far_k = (2, 3)
    order = far_k + (1, 0)

    def w2_copy(i):
        rows = pl.ds(i * w2rows, w2rows)
        return pltpu.make_async_copy(w2.at[rows, :], w2v.at[rows, :], w2_sem.at[i])

    def w1_copy(i):
        rows = pl.ds(i * blk, blk)
        return pltpu.make_async_copy(w1.at[rows, :], w1v.at[rows, :], w1_sem.at[i])

    def rows1(i, k):
        return pl.ds(pl.multiple_of(peer[k] * q1 + (i % halves) * rc, rc), rc)

    def cols1(i):
        return pl.ds(pl.multiple_of((i // halves) * cc, cc), cc)

    def rows2(i, k):
        return pl.ds(pl.multiple_of(peer[k] * q2 + i * rc, rc), rc)

    def acc1_copy(i, k):
        slot = i % 2
        return pltpu.make_async_copy(acc1.at[rows1(i, k), cols1(i)], stage.at[slot, k], st_sem.at[slot, k])

    def acc2_copy(i, k):
        slot = i % 2
        return pltpu.make_async_copy(acc2.at[rows2(i, k), :], stage.at[slot, k], st_sem.at[slot, k])

    def h_copy(t):
        rows = pl.ds((npp - 1 - s - t) * tok, tok)
        return pltpu.make_async_copy(hs.at[rows, :], hv.at[pl.ds(t * tok, tok), :], h_sem.at[t])

    def x_copy(t):
        rows = pl.ds((npp - 1 - s - t) * tok, tok)
        return pltpu.make_async_copy(xs.at[rows, :], xv.at[pl.ds(t * tok, tok), :], x_sem.at[t])

    dy_copy = pltpu.make_async_copy(dy, dyv, ld_sem.at[0])

    def used(t, start):
        @pl.when(t < npp - s)
        def _():
            start(t)

    for t in range(2):
        used(t, lambda t: h_copy(t).start())
    dy_copy.start()
    for i in range(3):
        w2_copy(i).start()

    barrier = pltpu.get_barrier_semaphore()
    for k in range(1, ndp):
        pl.semaphore_signal(barrier, inc=1, device_id={'dp': peer[k]}, device_id_type=MESH)
    for k in range(1, npp):
        pl.semaphore_signal(barrier, inc=1, device_id={'pp': (s + k) % npp}, device_id_type=MESH)

    for k in far_k:
        pl.semaphore_signal(barrier, inc=1, device_id={'pp': npp - 1 - s, 'dp': peer[k]}, device_id_type=MESH)

    rid = lax.broadcasted_iota(jnp.int32, (blk, blk), 0)
    cid = lax.broadcasted_iota(jnp.int32, (blk, blk), 1)
    ident[...] = jnp.where(rid == cid, 1.0, 0.0).astype(BF16)
    low = lax.broadcasted_iota(jnp.int32, (hb, half), 1) < tok

    def h_wait(t):
        @pl.when(t < npp - s)
        def _():
            h_copy(t).wait()

        @pl.when(t >= npp - s)
        def _():
            hv[t * tok:(t + 1) * tok, :] = jnp.zeros((tok, ff), BF16)

    def gelu_block(i, lanes):
        rows = slice(i * blk, (i + 1) * blk) if isinstance(i, int) else pl.ds(pl.multiple_of(i * blk, blk), blk)
        h = dot(ident[...], hv[lanes, rows], NT)
        h2 = h * h
        t = jnp.tanh(SQRT_2_OVER_PI * (h + 0.044715 * (h2 * h)))
        cdf = 0.5 * (1.0 + t)
        act[rows, lanes] = (h * cdf).astype(BF16)
        inner = SQRT_2_OVER_PI * (1.0 + (3.0 * 0.044715) * h2)
        slope[rows, lanes] = cdf + 0.5 * h * ((1.0 + t) * (1.0 - t)) * inner

    def gelu(hh, start, stop):
        def step(i, _):
            gelu_block(i, slice(hh * half, (hh + 1) * half))
            return 0

        with jax.named_scope('gelu'):
            lax.fori_loop(start, stop, step, 0, unroll=4)

    with jax.named_scope('hwait'):
        for t in range(2):
            h_wait(t)
        dy_copy.wait()
    for i in range(3, nw2):
        w2_copy(i).start()
    gt[...] = jnp.zeros_like(gt)
    for c in range(nblk):
        gt[c * blk:(c + 1) * blk, 0:tok] = dot(ident[...], dyv[:, c * blk:(c + 1) * blk], NT).astype(BF16)

    at0 = 1 - jnp.minimum(s, 1)

    def hop_copy(t, c):
        slot = t + (npp - 1 - t) * at0
        return pltpu.make_async_remote_copy(
            src_ref=gout.at[t, c], dst_ref=gin.at[slot, c], send_sem=hop_send.at[t, c], recv_sem=hop_recv.at[slot, c],
            device_id={'pp': (s - 1) * (1 - at0) + (npp - 1 - t) * at0}, device_id_type=MESH)

    def hop_wait(slot, c):
        pltpu.make_async_remote_copy(
            src_ref=gin.at[slot, c], dst_ref=gin.at[slot, c], send_sem=hop_send.at[0, c], recv_sem=hop_recv.at[slot, c],
            device_id={'pp': s}, device_id_type=MESH).wait_recv()

    def send_first(k):
        return pltpu.make_async_remote_copy(
            src_ref=first.at[k], dst_ref=recv2.at[k - 1, 0], send_sem=send2.at[k - 1, 0], recv_sem=recv2_sem.at[k - 1, 0],
            device_id={'dp': peer[k]}, device_id_type=MESH)


    def first_chunk():
        with jax.named_scope('first'):
            for k in order:
                acc2_copy(0, k).wait()
                rows = rows2(0, k)
                first[k] = (stage[0, k] + dot(act[rows, :], gt[...], NT)).astype(BF16)
                if k == order[1]:
                    send_first(order[0]).start()
                    send_first(order[1]).start()
            send_first(order[2]).start()
            for k in range(ndp):
                acc2_copy(2, k).start()

    def unpack(packed, c, t):
        lanes = slice((t // 2) * half, (t // 2 + 1) * half)
        v = packed.astype(F32)
        r = pltpu.roll(v, tok, 1)
        for b, (lo, hi) in enumerate(((v, r), (r, v))):
            rows = slice(c * blk + b * hb, c * blk + (b + 1) * hb)
            if t % 2 == 0:
                new = jnp.where(low, lo, 0.0)
            else:
                new = jnp.where(low, gt[rows, lanes].astype(F32), hi)
            gt[rows, lanes] = new.astype(BF16)

    for t in range(npp):
        lanes = slice((t // 2) * half, (t // 2 + 1) * half)

        @pl.when(t < npp - s)
        def _(t=t, lanes=lanes):
            if t == 0:
                gelu(0, 0, ff // blk // 2)
                for i in range(nblk):
                    w1_copy(i).start()
                gelu(0, ff // blk // 2, ff // blk)
                with jax.named_scope('u0'):
                    for i in range(ff // blk):
                        if i % (w2rows // blk) == 0:
                            w2_copy(i // (w2rows // blk)).wait()
                        rows = slice(i * blk, (i + 1) * blk)
                        u = dot(w2v[rows, :], gt[:, lanes], NN)
                        dht[rows, lanes] = (slope[rows, lanes] * u).astype(BF16)
                for t2 in range(2, npp):
                    used(t2, lambda t2: h_copy(t2).start())
                for t2 in range(npp):
                    used(t2, lambda t2: x_copy(t2).start())
                with jax.named_scope('barrier'):
                    pl.semaphore_wait(barrier, ndp - 1 + npp - 1 + len(far_k))
            else:
                groups = ((0,), (1,), (2, 3))
                for group in groups:
                    for c in group:
                        with jax.named_scope('gwait'):
                            hop_wait(t - 1, c)
                        unpack(gin[t - 1, c], c, t)
                    if t == npp - 1 and group == groups[-1]:
                        first_chunk()
                    krows = slice(group[0] * blk, (group[-1] + 1) * blk)

                    with jax.named_scope('u'):
                        for i in range(ff // mrows):
                            rows = slice(i * mrows, (i + 1) * mrows)
                            u = dot(w2v[rows, krows], gt[krows, lanes], NN)
                            if group != groups[0]:
                                u = uacc[rows, :] + u
                            if group != groups[-1]:
                                uacc[rows, :] = u
                            else:
                                dht[rows, lanes] = (slope[rows, lanes] * u).astype(BF16)

            def gx_dot(c, part):
                rows = slice(c * blk, (c + 1) * blk)
                k = slice(part * (ff // 2), (part + 1) * (ff // 2))
                return dot(w1v[rows, k], dht[k, lanes], NN)

            def gx_put(c, z):
                top, bot = z[:hb], z[hb:]
                if t % 2 == 0:
                    z = jnp.where(low, top, pltpu.roll(bot, tok, 1))
                else:
                    z = jnp.where(low, pltpu.roll(top, tok, 1), bot)
                gout[t, c] = z.astype(BF16)

                if t < npp - 1:
                    hop_copy(t, c).start()

            with jax.named_scope('gx'):
                last = None
                for c in range(nblk):
                    if t == 0 and c % 2 == 0:
                        w1_copy(c).wait()
                        w1_copy(c + 1).wait()
                    if t == 0 and c == 2:
                        for i in range(2):
                            for k in range(ndp):
                                acc2_copy(i, k).start()
                    z = gt[c * blk:(c + 1) * blk, lanes].astype(F32) + gx_dot(c, 0)
                    if c > 0:
                        gx_put(c - 1, last)
                    last = z + gx_dot(c, 1)
                gx_put(nblk - 1, last)

        if t == 0:
            @pl.when(s < npp - 2)
            def _():
                for t in range(2, npp):
                    h_wait(t)
                gelu(1, 0, ff // blk)

            @pl.when(s >= npp - 2)
            def _():
                act[:, half:] = jnp.zeros((ff, half), BF16)
                dht[:, half:] = jnp.zeros((ff, half), BF16)

    @pl.when(s > 0)
    def _():
        first_chunk()

    for t in range(npp):
        @pl.when(t < npp - s)
        def _():
            x_copy(t).wait()

        @pl.when(t >= npp - s)
        def _():
            xv[t * tok:(t + 1) * tok, :] = jnp.zeros((tok, dm), BF16)
    for c in range(nblk):
        rows = pl.ds(c * blk, blk)
        xt[rows, :] = dot(ident[...], xv[:, rows], NT).astype(BF16)

    def send2_copy(i, k):
        return pltpu.make_async_remote_copy(
            src_ref=w2v.at[rows2(i, k), :], dst_ref=recv2.at[k - 1, i],
            send_sem=send2.at[k - 1, i], recv_sem=recv2_sem.at[k - 1, i], device_id={'dp': peer[k]}, device_id_type=MESH)

    def send1_copy(i, k):
        return pltpu.make_async_remote_copy(
            src_ref=w1v.at[rows1(i, k), cols1(i)], dst_ref=recv1.at[k - 1, i],
            send_sem=send1.at[k - 1, i], recv_sem=recv1_sem.at[k - 1, i], device_id={'dp': peer[k]}, device_id_type=MESH)

    units = tuple((u, far_k[u // 2], u % 2) for u in range(4))

    def is_shed(u, stage):
        cond = jnp.bool_(False)
        for n, count in enumerate(shed):
            if u < count:
                cond = cond | (stage == n)
        return cond

    def unit_dst(k, b):
        return recv2.at[k - 1, 1, pl.ds(b * ru, ru), :]

    def unit_src(k, b):
        return w2v.at[pl.ds(pl.multiple_of(peer[k] * q2 + rc + b * ru, ru), ru), :]

    def unit_copy(u, k, b):
        return pltpu.make_async_remote_copy(
            src_ref=unit_src(k, b), dst_ref=unit_dst(k, b), send_sem=unit_send.at[u], recv_sem=unit_recv.at[u],
            device_id={'dp': peer[k]}, device_id_type=MESH)

    def shed_copy(u, k, b):
        return pltpu.make_async_remote_copy(
            src_ref=unit_src(k, b), dst_ref=relay.at[u], send_sem=unit_send.at[u], recv_sem=relay_recv.at[u],
            device_id={'pp': npp - 1 - s, 'dp': peer[k]}, device_id_type=MESH)

    def relay_copy(u, k, b):
        return pltpu.make_async_remote_copy(
            src_ref=relay.at[u], dst_ref=unit_dst(k, b), send_sem=relay_send.at[u], recv_sem=unit_recv.at[u],
            device_id={'pp': npp - 1 - s}, device_id_type=MESH)

    def send_unit(u, k, b):
        cond = is_shed(u, s)

        @pl.when(cond)
        def _():
            shed_copy(u, k, b).start()

        @pl.when(jnp.logical_not(cond))
        def _():
            unit_copy(u, k, b).start()

    def a2_add(i):
        for k in order:
            acc2_copy(i, k).wait()
            rows = rows2(i, k)
            w2v[rows, :] = (stage[i % 2, k] + dot(act[rows, :], gt[...], NT)).astype(BF16)

    def a2_next(i):
        @pl.when(i + 2 < nchunk)
        def _():
            for k in range(ndp):
                acc2_copy(i + 2, k).start()

        @pl.when(i + 2 >= nchunk)
        def _():
            for k in range(ndp):
                acc1_copy(i + 2 - nchunk, k).start()

    def a2_step(i, _):
        a2_add(i)
        for k in order[:-1]:
            send2_copy(i, k).start()
        a2_next(i)
        return 0

    with jax.named_scope('a2'):
        a2_add(1)
        for unit in units:
            send_unit(*unit)
        send2_copy(1, 1).start()
        a2_next(jnp.int32(1))
        lax.fori_loop(2, nchunk, a2_step, 0)

    with jax.named_scope('relay'):
        for u, k, b in units:
            @pl.when(is_shed(u, npp - 1 - s))
            def _():
                pltpu.make_async_remote_copy(
                    src_ref=relay.at[u], dst_ref=relay.at[u], send_sem=relay_send.at[u], recv_sem=relay_recv.at[u],
                    device_id={'pp': npp - 1 - s}, device_id_type=MESH).wait_recv()
                relay_copy(u, k, b).start()

    def a1_step(i, _):
        slot = i % 2
        for k in order:
            acc1_copy(i, k).wait()
            w1v[rows1(i, k), cols1(i)] = (
                stage[slot, k] + dot(xt[rows1(i, k), :], dht[cols1(i), :], NT)).astype(BF16)
        for k in order[:-1]:
            send1_copy(i, k).start()

        @pl.when(i + 2 < nchunk)
        def _():
            for k in range(ndp):
                acc1_copy(i + 2, k).start()
        return 0

    with jax.named_scope('a1'):
        lax.fori_loop(0, nchunk, a1_step, 0)

    def put_dx(packed, c, e):
        v = packed.astype(F32)
        r = pltpu.roll(v, tok, 1)
        col = jnp.concatenate([v, r], axis=0).astype(BF16)
        dx[:, c * blk:(c + 1) * blk] = dot(ident[:tok, :half], col, NT).astype(BF16)

    for c in range(nblk):
        @pl.when(s == 0)
        def _():
            put_dx(gout[npp - 1, c], c, 0)

        @pl.when(s > 0)
        def _():
            hop_wait(npp - 1, c)
            put_dx(gin[npp - 1, c], c, 0)

    scale = 1.0 / ndp

    def r2_sum(i, own):
        for k in range(1, ndp):
            own = own + recv2[k - 1, i].astype(F32)
        g2[pl.ds(pl.multiple_of(i * rc, rc), rc), :] = own * scale

    for k in order[:-1]:
        send_first(k).wait()
    r2_sum(0, first[0].astype(F32))

    for u, k, b in units:
        unit_copy(u, k, b).wait()

        @pl.when(is_shed(u, npp - 1 - s))
        def _():
            relay_copy(u, k, b).wait_send()
    send2_copy(1, 1).wait()
    r2_sum(1, w2v[rows2(1, 0), :].astype(F32))

    def r2_step(i, _):
        with jax.named_scope('r2wait'):
            for k in order[:-1]:
                send2_copy(i, k).wait()
        r2_sum(i, w2v[rows2(i, 0), :].astype(F32))
        return 0

    lax.fori_loop(2, nchunk, r2_step, 0)

    def r1_step(i, _):
        with jax.named_scope('r1wait'):
            for k in order[:-1]:
                send1_copy(i, k).wait()
        with jax.named_scope('r1sum'):
            tot = w1v[rows1(i, 0), cols1(i)].astype(F32)
            for k in range(1, ndp):
                tot = tot + recv1[k - 1, i].astype(F32)
            g1[pl.ds(pl.multiple_of((i % halves) * rc, rc), rc), cols1(i)] = tot * scale
        return 0

    lax.fori_loop(0, nchunk, r1_step, 0)

    with jax.named_scope('tail'):
        for t in range(npp - 1):
            @pl.when(t < npp - s)
            def _():
                for c in range(nblk):
                    hop_copy(t, c).wait_send()


def put(g1, g2, dx, o1, o2, o3, sems):
    pieces = 4
    copies = []
    for n, (src, dst) in enumerate(((g1, o1), (g2, o2))):
        size = src.shape[0] // pieces
        for i in range(pieces):
            rows = pl.ds(i * size, size)
            copies.append(pltpu.make_async_copy(src.at[rows, :], dst.at[rows, :], sems.at[n * pieces + i]))
    copies.append(pltpu.make_async_copy(dx, o3, sems.at[2 * pieces]))
    for copy in copies:
        copy.start()
    for copy in copies:
        copy.wait()


def solution(mesh):
    npp = mesh.shape['pp']
    ndp = mesh.shape['dp']

    def body(dy, xs, hs, w1, w2, acc1, acc2):
        tok = dy.shape[1]
        dm, ff = w1.shape[2:]
        ntok = npp * tok
        nchunk = 8
        blk = 256
        nblk = dm // blk
        q1, q2 = dm // ndp, ff // ndp
        rc, cc = q2 // nchunk, dm
        dma = pltpu.SemaphoreType.DMA
        any_spec = pl.BlockSpec(memory_space=pl.ANY)
        vmem = pl.BlockSpec(memory_space=pltpu.VMEM)
        shapes = ((q1, ff), F32), ((q2, dm), F32), ((tok, dm), BF16)
        outs = pl.pallas_call(
            functools.partial(kernel, npp, ndp, tok, nchunk),
            out_shape=tuple(pltpu.VMEM(shape, dtype) for shape, dtype in shapes),
            in_specs=[any_spec] * 7,
            out_specs=(vmem,) * 3,
            scratch_shapes=[
                pltpu.VMEM((dm, ff), BF16), pltpu.VMEM((ff, dm), BF16),
                pltpu.VMEM((ndp - 1, nchunk, rc, cc), BF16), pltpu.VMEM((ndp - 1, nchunk, rc, cc), BF16),
                pltpu.VMEM((ntok, ff), BF16), pltpu.VMEM((ntok, dm), BF16),
                pltpu.VMEM((ff, ntok), BF16), pltpu.VMEM((ff, ntok), F32), pltpu.VMEM((ff, ntok), BF16),
                pltpu.VMEM((dm, ntok), BF16), pltpu.VMEM((dm, ntok), BF16), pltpu.VMEM((ff, 2 * tok), F32),
                pltpu.VMEM((ndp, rc, cc), BF16),
                pltpu.VMEM((npp, nblk, blk // 2, 2 * tok), BF16), pltpu.VMEM((npp, nblk, blk // 2, 2 * tok), BF16),
                pltpu.VMEM((4, rc // 2, cc), BF16), pltpu.VMEM((blk, blk), BF16),
                pltpu.VMEM((2, ndp, rc, cc), F32), pltpu.VMEM((tok, dm), BF16),
                dma((1,)), dma((npp,)), dma((npp,)), dma((8,)), dma((nblk,)), dma((2, ndp)),
                dma((npp - 1, nblk)), dma((npp, nblk)),
                dma((ndp - 1, nchunk)), dma((ndp - 1, nchunk)), dma((ndp - 1, nchunk)), dma((ndp - 1, nchunk)),
                dma((4,)), dma((4,)), dma((4,)), dma((4,)),
            ],
            compiler_params=pltpu.CompilerParams(
                collective_id=0, has_side_effects=True, vmem_limit_bytes=52 * 1024 * 1024),
        )(dy[0], xs.reshape(ntok, dm), hs.reshape(ntok, ff), w1[0, 0], w2[0, 0], acc1[0, 0, 0], acc2[0, 0, 0])
        r1, r2, dx = pl.pallas_call(
            put,
            out_shape=tuple(jax.ShapeDtypeStruct(shape, dtype) for shape, dtype in shapes),
            in_specs=[any_spec] * 3,
            out_specs=(any_spec,) * 3,
            scratch_shapes=[dma((9,))],
            compiler_params=pltpu.CompilerParams(vmem_limit_bytes=1024 * 1024),
        )(*outs)
        return r1[None, None], r2[None, None], dx[None]

    spec_row = P(('grp', 'pp'), 'dp', None)
    spec_saved = P(('grp', 'pp'), None, None, 'dp', None)
    spec_w = P(('grp', 'pp'), None, None, None)
    spec_acc = P(('grp', 'pp'), 'dp', None, None, None)
    spec_g = P(('grp', 'pp'), None, 'dp', None)
    return jax.shard_map(body, mesh=mesh, in_specs=(spec_row, spec_saved, spec_saved, spec_w, spec_w, spec_acc, spec_acc), out_specs=(spec_g, spec_g, spec_row), check_vma=False)
```

```python
import functools

import jax
import jax.numpy as jnp
from jax import lax
from jax.experimental import pallas as pl
from jax.experimental.pallas import tpu as pltpu
from jax.sharding import PartitionSpec as P

MESH = pl.DeviceIdType.MESH
EARLY = (3,)
VMEM_LIMIT = 53 * 1024 * 1024
NN = (((1,), (0,)), ((), ()))
NT = (((1,), (1,)), ((), ()))
SQRT_2_OVER_PI = 0.7978845608028654
BF16 = jnp.bfloat16
F32 = jnp.float32


def dot(a, b, dims):
    return lax.dot_general(a, b, dims, preferred_element_type=F32)


def kernel(npp, ndp, tok, nchunk, dy, xs, hs, w1, w2, acc1, acc2, g1, g2, dx,
           w1v, w2v, recv1, recv2, hv, xv, act, slope, dht, xt, gt, uacc, first, gin, gout, relay, ident,
           stage1, stage2, early_acc, early_act, early_g, dyv,
           ld_sem, h_sem, x_sem, w2_sem, w1_sem, st1_sem, st2_sem, hop_send, hop_recv,
           send1, recv1_sem, send2, recv2_sem, far_recv, unit_recv, relay_send, relay_recv,
           early_send, early_recv):
    s = lax.axis_index('pp')
    p = lax.axis_index('dp')
    dm, ff = w1v.shape
    blk = ident.shape[0]
    half = 2 * tok
    hb = blk // 2
    nw2 = w2_sem.shape[0]
    w2rows = ff // nw2
    nblk = dm // blk
    q1 = dm // ndp
    q2 = ff // ndp
    rc1, cc1 = stage1.shape[2:]
    rc, cc = first.shape[1:]
    halves = q1 // rc1
    across = dm // cc
    mrows = 1024
    ru = rc // 4
    shed = (5, 2)
    early = tuple(zip((nchunk - 1, nchunk - 2), EARLY))

    far = (p + 2) % ndp
    peer = (p, p + 1 - 2 * (p % 2), far, far + 1 - 2 * (far % 2))

    far_k = (2, 3)
    order = far_k + (1, 0)

    def w2_copy(i):
        rows = pl.ds(i * w2rows, w2rows)
        return pltpu.make_async_copy(w2.at[rows, :], w2v.at[rows, :], w2_sem.at[i])

    def w1_copy(i):
        rows = pl.ds(i * blk, blk)
        return pltpu.make_async_copy(w1.at[rows, :], w1v.at[rows, :], w1_sem.at[i])

    def rows1(i, k):
        return pl.ds(pl.multiple_of(peer[k] * q1 + (i % halves) * rc1, rc1), rc1)

    def cols1(i):
        return pl.ds(pl.multiple_of((i // halves) * cc1, cc1), cc1)

    def rows2(i, k):
        return pl.ds(pl.multiple_of(peer[k] * q2 + (i // across) * rc, rc), rc)

    def cols2(i):
        return pl.ds(pl.multiple_of((i % across) * cc, cc), cc)

    def acc1_copy(i, k):
        return pltpu.make_async_copy(acc1.at[rows1(i, k), cols1(i)], stage1.at[i % 2, k], st1_sem.at[i % 2])

    def acc1_wait(i):
        pltpu.make_async_copy(stage1.at[i % 2], stage1.at[i % 2], st1_sem.at[i % 2]).wait()

    def slot2(i, k, n=1):
        return pl.ds(pl.multiple_of(((i % 2) * ndp + k) * rc, rc), n * rc)

    def acc2_copy(i, k):
        return pltpu.make_async_copy(acc2.at[rows2(i, k), cols2(i)], slope.at[slot2(i, k), :], st2_sem.at[i % 2])

    def acc2_wait(i):
        span = slope.at[slot2(i, 0, ndp), :]
        pltpu.make_async_copy(span, span, st2_sem.at[i % 2]).wait()

    def first_copy(k):
        return pltpu.make_async_copy(acc2.at[rows2(0, k), cols2(0)], stage2.at[k], st2_sem.at[2])

    def h_copy(t):
        rows = pl.ds((npp - 1 - s - t) * tok, tok)
        return pltpu.make_async_copy(hs.at[rows, :], hv.at[pl.ds(t * tok, tok), :], h_sem.at[t])

    def x_copy(t):
        rows = pl.ds((npp - 1 - s - t) * tok, tok)
        return pltpu.make_async_copy(xs.at[rows, :], xv.at[pl.ds(t * tok, tok), :], x_sem.at[t])

    dy_copy = pltpu.make_async_copy(dy, dyv, ld_sem.at[0])

    def used(t, start):
        @pl.when(t < npp - s)
        def _():
            start(t)

    for t in range(2):
        used(t, lambda t: h_copy(t).start())
    dy_copy.start()
    for i in range(1):
        w2_copy(i).start()

    barrier = pltpu.get_barrier_semaphore()
    for k in range(1, ndp):
        pl.semaphore_signal(barrier, inc=1, device_id={'dp': peer[k]}, device_id_type=MESH)
    for k in range(1, npp):
        pl.semaphore_signal(barrier, inc=1, device_id={'pp': (s + k) % npp}, device_id_type=MESH)

    for k in far_k:
        pl.semaphore_signal(barrier, inc=1, device_id={'pp': npp - 1 - s, 'dp': peer[k]}, device_id_type=MESH)

    rid = lax.broadcasted_iota(jnp.int32, (blk, blk), 0)
    cid = lax.broadcasted_iota(jnp.int32, (blk, blk), 1)
    ident[...] = jnp.where(rid == cid, 1.0, 0.0).astype(BF16)
    low = lax.broadcasted_iota(jnp.int32, (hb, half), 1) < tok

    def h_wait(t):
        @pl.when(t < npp - s)
        def _():
            h_copy(t).wait()

        @pl.when(t >= npp - s)
        def _():
            hv[t * tok:(t + 1) * tok, :] = jnp.zeros((tok, ff), BF16)

    def gelu_block(i, lanes):
        rows = slice(i * blk, (i + 1) * blk) if isinstance(i, int) else pl.ds(pl.multiple_of(i * blk, blk), blk)
        h = dot(ident[...], hv[lanes, rows], NT)
        h2 = h * h
        t = jnp.tanh(h * (SQRT_2_OVER_PI + (SQRT_2_OVER_PI * 0.044715) * h2))
        cdf = 0.5 + 0.5 * t
        a = h * cdf
        act[rows, lanes] = a.astype(BF16)
        slope[rows, lanes] = cdf + (a * (1.0 - cdf)) * (2.0 * SQRT_2_OVER_PI + (6.0 * SQRT_2_OVER_PI * 0.044715) * h2)

    def gelu(hh, start, stop):
        def step(i, _):
            gelu_block(i, slice(hh * half, (hh + 1) * half))
            return 0

        with jax.named_scope('gelu'):
            lax.fori_loop(start, stop, step, 0, unroll=4)

    with jax.named_scope('hwait'):
        for t in range(2):
            h_wait(t)
        dy_copy.wait()
    for i in range(1, nw2):
        w2_copy(i).start()
    gt[...] = jnp.zeros_like(gt)

    @pl.when(s >= npp - 2)
    def _():
        early_act[:, half:] = jnp.zeros((rc, half), BF16)
        for n in range(len(early)):
            early_g[n, :, half:] = jnp.zeros((cc, half), BF16)

    for c in range(nblk):
        gt[c * blk:(c + 1) * blk, 0:tok] = dot(ident[...], dyv[:, c * blk:(c + 1) * blk], NT).astype(BF16)

    at0 = 1 - jnp.minimum(s, 1)

    def hop_copy(t, c):
        slot = t + (npp - 1 - t) * at0
        return pltpu.make_async_remote_copy(
            src_ref=gout.at[t, c], dst_ref=gin.at[slot, c], send_sem=hop_send.at[t], recv_sem=hop_recv.at[slot, c],
            device_id={'pp': (s - 1) * (1 - at0) + (npp - 1 - t) * at0}, device_id_type=MESH)

    def hop_wait(slot, c):
        pltpu.make_async_remote_copy(
            src_ref=gin.at[slot, c], dst_ref=gin.at[slot, c], send_sem=hop_send.at[0], recv_sem=hop_recv.at[slot, c],
            device_id={'pp': s}, device_id_type=MESH).wait_recv()

    slot_of = {1: 0, 3: 1, 2: 2}

    def sems2(i, k):
        return dict(send_sem=send2.at[1 if k == 2 else 0], recv_sem=far_recv.at[i] if k == 2 else recv2_sem.at[i],
                    device_id={'dp': peer[k]}, device_id_type=MESH)

    def send_first(k):
        return pltpu.make_async_remote_copy(src_ref=first.at[k], dst_ref=recv2.at[slot_of[k], 0], **sems2(0, k))

    hl = (slice(0, half), slice(half, 2 * half))

    def early_on(n):
        return s < early[n][1]

    def early_copy(what, n, hh, cond_start=True):
        i = early[n][0]
        if what == 'acc':
            src, dst, q = acc2.at[rows2(i, 2), cols2(i)], early_acc.at[n], n
        elif what == 'act':
            src, dst, q = act.at[rows2(i, 2), hl[hh]], early_act.at[:, hl[hh]], 2 + hh
        else:
            src, dst, q = gt.at[cols2(i), hl[hh]], early_g.at[n, :, hl[hh]], 4 + 2 * n + hh
        return pltpu.make_async_remote_copy(
            src_ref=src, dst_ref=dst, send_sem=early_send.at[q], recv_sem=early_recv.at[q],
            device_id={'dp': peer[2]}, device_id_type=MESH)

    def early_start():
        for n in range(len(early)):
            @pl.when(early_on(n))
            def _():
                early_copy('acc', n, 0).start()
                if n == 0:
                    early_copy('act', 0, 0).start()

    def early_gt(hh, cond=None):
        for n in range(len(early)):
            @pl.when(early_on(n) if cond is None else early_on(n) & cond)
            def _():
                early_copy('g', n, hh).start()


    def first_chunk():
        with jax.named_scope('first'):
            pltpu.make_async_copy(stage2, stage2, st2_sem.at[2]).wait()
            for k in order:
                first[k] = (stage2[k] + dot(act[rows2(0, k), :], gt[0:cc, :], NT)).astype(BF16)
                if k == order[1]:
                    send_first(order[0]).start()
                    send_first(order[1]).start()
            send_first(order[2]).start()

    def unpack(packed, c, t):
        lanes = slice((t // 2) * half, (t // 2 + 1) * half)
        v = packed.astype(F32)
        r = pltpu.roll(v, tok, 1)
        for b, (lo, hi) in enumerate(((v, r), (r, v))):
            rows = slice(c * blk + b * hb, c * blk + (b + 1) * hb)
            if t % 2 == 0:
                new = jnp.where(low, lo, 0.0)
            else:
                new = jnp.where(low, gt[rows, lanes].astype(F32), hi)
            gt[rows, lanes] = new.astype(BF16)

    for t in range(npp):
        lanes = slice((t // 2) * half, (t // 2 + 1) * half)

        @pl.when(t < npp - s)
        def _(t=t, lanes=lanes):
            if t == 0:
                gelu(0, 0, ff // blk // 2)
                for i in range(nblk):
                    w1_copy(i).start()
                gelu(0, ff // blk // 2, ff // blk)
                with jax.named_scope('barrier'):
                    pl.semaphore_wait(barrier, ndp - 1 + npp - 1 + len(far_k))
                early_start()
                with jax.named_scope('u0'):
                    for part in range(2):
                        for b in range(nw2 // 2):
                            w2_copy(part * (nw2 // 2) + b).wait()
                        for c in range(nblk):
                            krows = slice(c * blk, (c + 1) * blk)
                            for i in range(ff // mrows // 2):
                                rows = slice(part * (ff // 2) + i * mrows, part * (ff // 2) + (i + 1) * mrows)
                                u = dot(w2v[rows, krows], gt[krows, lanes], NN)
                                if c > 0:
                                    u = uacc[rows, :] + u
                                if c < nblk - 1:
                                    uacc[rows, :] = u
                                else:
                                    dht[rows, lanes] = (slope[rows, lanes] * u).astype(BF16)
                for t2 in range(2, npp):
                    used(t2, lambda t2: h_copy(t2).start())
                for t2 in range(npp):
                    used(t2, lambda t2: x_copy(t2).start())
            else:
                groups = ((0,), (1,), (2, 3))
                for group in groups:
                    for c in group:
                        with jax.named_scope('gwait'):
                            hop_wait(t - 1, c)
                        unpack(gin[t - 1, c], c, t)
                    if group == groups[-1]:
                        if t == npp - 1:
                            first_chunk()
                            early_gt(1)
                        elif t == npp - 2:
                            early_gt(1, s == 1)
                        elif t == 1:
                            early_gt(0)
                    krows = slice(group[0] * blk, (group[-1] + 1) * blk)

                    with jax.named_scope('u'):
                        for i in range(ff // mrows):
                            rows = slice(i * mrows, (i + 1) * mrows)
                            u = dot(w2v[rows, krows], gt[krows, lanes], NN)
                            if group != groups[0]:
                                u = uacc[rows, :] + u
                            if group != groups[-1]:
                                uacc[rows, :] = u
                            else:
                                dht[rows, lanes] = (slope[rows, lanes] * u).astype(BF16)

            def gx_dot(c, part):
                rows = slice(c * blk, (c + 1) * blk)
                k = slice(part * (ff // 2), (part + 1) * (ff // 2))
                return dot(w1v[rows, k], dht[k, lanes], NN)

            def gx_put(c, z):
                top, bot = z[:hb], z[hb:]
                if t % 2 == 0:
                    z = jnp.where(low, top, pltpu.roll(bot, tok, 1))
                else:
                    z = jnp.where(low, pltpu.roll(top, tok, 1), bot)
                gout[t, c] = z.astype(BF16)

                if t < npp - 1:
                    hop_copy(t, c).start()

            with jax.named_scope('gx'):
                last = None
                for c in range(nblk):
                    if t == 0 and c % 2 == 0:
                        w1_copy(c).wait()
                        w1_copy(c + 1).wait()
                    if t == 0 and c == 2:
                        for k in range(ndp):
                            first_copy(k).start()
                        for i in range(2):
                            for k in range(ndp):
                                acc1_copy(i, k).start()
                    z = gt[c * blk:(c + 1) * blk, lanes].astype(F32) + gx_dot(c, 0)
                    if c > 0:
                        gx_put(c - 1, last)
                    last = z + gx_dot(c, 1)
                gx_put(nblk - 1, last)

        if t == 0:
            @pl.when(s < npp - 2)
            def _():
                for t in range(2, npp):
                    h_wait(t)
                gelu(1, 0, ff // blk)

                @pl.when(early_on(0))
                def _():
                    early_copy('act', 0, 1).start()

            @pl.when(s >= npp - 2)
            def _():
                act[:, half:] = jnp.zeros((ff, half), BF16)
                dht[:, half:] = jnp.zeros((ff, half), BF16)

    for i in range(1, 3):
        for k in range(ndp):
            acc2_copy(i, k).start()

    @pl.when(s > 0)
    def _():
        first_chunk()

    for t in range(npp):
        @pl.when(t < npp - s)
        def _():
            x_copy(t).wait()

        @pl.when(t >= npp - s)
        def _():
            xv[t * tok:(t + 1) * tok, :] = jnp.zeros((tok, dm), BF16)
    for c in range(nblk):
        rows = pl.ds(c * blk, blk)
        xt[rows, :] = dot(ident[...], xv[:, rows], NT).astype(BF16)

    def send2_copy(i, k):
        return pltpu.make_async_remote_copy(
            src_ref=w2v.at[rows2(i, k), cols2(i)], dst_ref=recv2.at[slot_of[k], i], **sems2(i, k))

    def send1_copy(i, k):
        return pltpu.make_async_remote_copy(
            src_ref=w1v.at[rows1(i, k), cols1(i)], dst_ref=recv1.at[i, k - 1],
            send_sem=send1.at[0], recv_sem=recv1_sem.at[i], device_id={'dp': peer[k]}, device_id_type=MESH)

    units = tuple((u, far_k[u // 4], u % 4) for u in range(8))

    def is_shed(u, stage):
        cond = jnp.bool_(False)
        for n, count in enumerate(shed):
            if u < count:
                cond = cond | (stage == n)
        return cond

    def unit_dst(k, b):
        return recv2.at[slot_of[k], 1, pl.ds(b * ru, ru), :]

    def unit_src(k, b):
        return w2v.at[pl.ds(pl.multiple_of(peer[k] * q2 + b * ru, ru), ru), cols2(1)]

    def unit_copy(u, k, b):
        return pltpu.make_async_remote_copy(
            src_ref=unit_src(k, b), dst_ref=unit_dst(k, b), send_sem=send2.at[1 if k == 2 else 0], recv_sem=unit_recv.at[u],
            device_id={'dp': peer[k]}, device_id_type=MESH)

    def shed_copy(u, k, b):
        return pltpu.make_async_remote_copy(
            src_ref=unit_src(k, b), dst_ref=relay.at[u], send_sem=send2.at[1 if k == 2 else 0], recv_sem=relay_recv.at[u],
            device_id={'pp': npp - 1 - s, 'dp': peer[k]}, device_id_type=MESH)

    def relay_copy(u, k, b):
        return pltpu.make_async_remote_copy(
            src_ref=relay.at[u], dst_ref=unit_dst(k, b), send_sem=relay_send.at[u], recv_sem=unit_recv.at[u],
            device_id={'pp': npp - 1 - s}, device_id_type=MESH)

    def send_unit(u, k, b):
        cond = is_shed(u, s)

        @pl.when(cond)
        def _():
            shed_copy(u, k, b).start()

        @pl.when(jnp.logical_not(cond))
        def _():
            unit_copy(u, k, b).start()

    def a2_add(i):
        acc2_wait(i)
        for k in order:
            w2v[rows2(i, k), cols2(i)] = (
                slope[slot2(i, k), :] + dot(act[rows2(i, k), :], gt[cols2(i), :], NT)).astype(BF16)

    def a2_next(i):
        @pl.when(i + 2 < nchunk)
        def _():
            for k in range(ndp):
                acc2_copy(i + 2, k).start()

    plain = nchunk - len(early)

    def a2_step(i, _):
        a2_add(i)
        for k in order[:-1]:
            send2_copy(i, k).start()
        a2_next(i)
        return 0

    def far_copy(n):
        i = early[n][0]
        return pltpu.make_async_remote_copy(
            src_ref=w2v.at[rows2(i, 2), cols2(i)], dst_ref=recv2.at[slot_of[2], i],
            send_sem=send2.at[2 + n], recv_sem=far_recv.at[i], device_id={'dp': peer[2]}, device_id_type=MESH)

    with jax.named_scope('a2'):
        a2_add(1)
        for unit in units:
            send_unit(*unit)
        send2_copy(1, 1).start()
        a2_next(jnp.int32(1))
        lax.fori_loop(2, plain, a2_step, 0)
        for n in reversed(range(len(early))):
            i = early[n][0]
            a2_add(i)

            @pl.when(jnp.logical_not(early_on(n)))
            def _():
                far_copy(n).start()
            for k in (3, 1):
                send2_copy(i, k).start()

    with jax.named_scope('relay'):
        for u, k, b in units:
            @pl.when(is_shed(u, npp - 1 - s))
            def _():
                pltpu.make_async_remote_copy(
                    src_ref=relay.at[u], dst_ref=relay.at[u], send_sem=relay_send.at[u], recv_sem=relay_recv.at[u],
                    device_id={'pp': npp - 1 - s}, device_id_type=MESH).wait_recv()
                relay_copy(u, k, b).start()

    def a1_step(i, _):
        acc1_wait(i)
        for k in order:
            w1v[rows1(i, k), cols1(i)] = (
                stage1[i % 2, k] + dot(xt[rows1(i, k), :], dht[cols1(i), :], NT)).astype(BF16)
        for k in order[:-1]:
            send1_copy(i, k).start()

        @pl.when(i + 2 < nchunk)
        def _():
            for k in range(ndp):
                acc1_copy(i + 2, k).start()
        return 0

    with jax.named_scope('a1'):
        lax.fori_loop(0, nchunk, a1_step, 0)

    def put_dx(packed, c, e):
        v = packed.astype(F32)
        r = pltpu.roll(v, tok, 1)
        col = jnp.concatenate([v, r], axis=0).astype(BF16)
        dx[:, c * blk:(c + 1) * blk] = dot(ident[:tok, :half], col, NT).astype(BF16)

    for c in range(nblk):
        @pl.when(s == 0)
        def _():
            put_dx(gout[npp - 1, c], c, 0)

        @pl.when(s > 0)
        def _():
            hop_wait(npp - 1, c)
            put_dx(gin[npp - 1, c], c, 0)

    scale = 1.0 / ndp

    def all_of(ref, sem):
        return pltpu.make_async_copy(ref, ref, sem)

    def r2_sum(i, own):
        for k in range(1, ndp):
            own = own + recv2[slot_of[k], i].astype(F32)
        rows = pl.ds(pl.multiple_of((i // across) * rc, rc), rc)
        g2[rows, cols2(i)] = own * scale

    def r2_wait(i):
        with jax.named_scope('r2wait'):
            all_of(recv2.at[0:2, i], recv2_sem.at[i]).wait()
            all_of(recv2.at[2, i], far_recv.at[i]).wait()

    r2_wait(0)
    r2_sum(0, first[0].astype(F32))

    for u, k, b in units:
        all_of(relay.at[u], unit_recv.at[u]).wait()
    all_of(recv2.at[0, 1], recv2_sem.at[1]).wait()
    r2_sum(1, w2v[rows2(1, 0), cols2(1)].astype(F32))

    def r2_step(i, _):
        r2_wait(i)
        r2_sum(i, w2v[rows2(i, 0), cols2(i)].astype(F32))
        return 0

    lax.fori_loop(2, plain, r2_step, 0)

    for n in reversed(range(len(early))):
        i = early[n][0]

        @pl.when(early_on(n))
        def _():
            early_copy('acc', n, 0).wait()
            for hh in range(2):
                if hh == 0:
                    if n == 0:
                        early_copy('act', n, hh).wait()
                    early_copy('g', n, hh).wait()
                else:
                    @pl.when(s < npp - 2)
                    def _():
                        if n == 0:
                            early_copy('act', n, hh).wait()
                        early_copy('g', n, hh).wait()
            recv2[slot_of[2], i] = (early_acc[n] + dot(early_act[...], early_g[n], NT)).astype(BF16)

        @pl.when(jnp.logical_not(early_on(n)))
        def _():
            far_copy(n).wait()
        with jax.named_scope('r2wait'):
            all_of(recv2.at[0:2, i], recv2_sem.at[i]).wait()
        r2_sum(i, w2v[rows2(i, 0), cols2(i)].astype(F32))

    def r1_step(i, _):
        with jax.named_scope('r1wait'):
            all_of(recv1.at[i], recv1_sem.at[i]).wait()
        with jax.named_scope('r1sum'):
            tot = w1v[rows1(i, 0), cols1(i)].astype(F32)
            for k in range(1, ndp):
                tot = tot + recv1[i, k - 1].astype(F32)
            g1[pl.ds(pl.multiple_of((i % halves) * rc1, rc1), rc1), cols1(i)] = tot * scale
        return 0

    lax.fori_loop(0, nchunk, r1_step, 0)

    with jax.named_scope('tail'):
        all_of(recv1, send1.at[0]).wait()
        all_of(recv2.at[0:2], send2.at[0]).wait()
        all_of(recv2.at[2, 0:plain], send2.at[1]).wait()
        for u, k, b in units:
            @pl.when(is_shed(u, npp - 1 - s))
            def _():
                relay_copy(u, k, b).wait_send()
        for t in range(npp - 1):
            @pl.when(t < npp - s)
            def _():
                all_of(gout.at[t], hop_send.at[t]).wait()


def put(g1, g2, dx, o1, o2, o3, sems):
    pieces = 4
    copies = []
    for n, (src, dst) in enumerate(((g1, o1), (g2, o2))):
        size = src.shape[0] // pieces
        for i in range(pieces):
            rows = pl.ds(i * size, size)
            copies.append(pltpu.make_async_copy(src.at[rows, :], dst.at[rows, :], sems.at[n * pieces + i]))
    copies.append(pltpu.make_async_copy(dx, o3, sems.at[2 * pieces]))
    for copy in copies:
        copy.start()
    for copy in copies:
        copy.wait()


def solution(mesh):
    npp = mesh.shape['pp']
    ndp = mesh.shape['dp']

    def body(dy, xs, hs, w1, w2, acc1, acc2):
        tok = dy.shape[1]
        dm, ff = w1.shape[2:]
        ntok = npp * tok
        nchunk = 8
        blk = 256
        nblk = dm // blk
        q1, q2 = dm // ndp, ff // ndp
        rc1, cc1 = q1 // 2, ff // (nchunk // 2)
        rc, cc = q2 // 2, dm // (nchunk // 2)
        dma = pltpu.SemaphoreType.DMA
        any_spec = pl.BlockSpec(memory_space=pl.ANY)
        vmem = pl.BlockSpec(memory_space=pltpu.VMEM)
        shapes = ((q1, ff), F32), ((q2, dm), F32), ((tok, dm), BF16)
        outs = pl.pallas_call(
            functools.partial(kernel, npp, ndp, tok, nchunk),
            out_shape=tuple(pltpu.VMEM(shape, dtype) for shape, dtype in shapes),
            in_specs=[any_spec] * 7,
            out_specs=(vmem,) * 3,
            scratch_shapes=[
                pltpu.VMEM((dm, ff), BF16), pltpu.VMEM((ff, dm), BF16),
                pltpu.VMEM((nchunk, ndp - 1, rc1, cc1), BF16), pltpu.VMEM((ndp - 1, nchunk, rc, cc), BF16),
                pltpu.VMEM((ntok, ff), BF16), pltpu.VMEM((ntok, dm), BF16),
                pltpu.VMEM((ff, ntok), BF16), pltpu.VMEM((ff, ntok), F32), pltpu.VMEM((ff, ntok), BF16),
                pltpu.VMEM((dm, ntok), BF16), pltpu.VMEM((dm, ntok), BF16), pltpu.VMEM((ff, 2 * tok), F32),
                pltpu.VMEM((ndp, rc, cc), BF16),
                pltpu.VMEM((npp, nblk, blk // 2, 2 * tok), BF16), pltpu.VMEM((npp, nblk, blk // 2, 2 * tok), BF16),
                pltpu.VMEM((8, rc // 4, cc), BF16), pltpu.VMEM((blk, blk), BF16),
                pltpu.VMEM((2, ndp, rc1, cc1), F32), pltpu.VMEM((ndp, rc, cc), F32),
                pltpu.VMEM((len(EARLY), rc, cc), F32), pltpu.VMEM((rc, ntok), BF16), pltpu.VMEM((len(EARLY), cc, ntok), BF16),
                pltpu.VMEM((tok, dm), BF16),
                dma((1,)), dma((npp,)), dma((npp,)), dma((8,)), dma((nblk,)), dma((2,)), dma((3,)),
                dma((npp - 1,)), dma((npp, nblk)),
                dma((1,)), dma((nchunk,)), dma((4,)), dma((nchunk,)), dma((nchunk,)), dma((8,)), dma((8,)), dma((8,)),
                dma((8,)), dma((8,)),
            ],
            compiler_params=pltpu.CompilerParams(
                collective_id=0, has_side_effects=True, vmem_limit_bytes=VMEM_LIMIT),
        )(dy[0], xs.reshape(ntok, dm), hs.reshape(ntok, ff), w1[0, 0], w2[0, 0], acc1[0, 0, 0], acc2[0, 0, 0])
        r1, r2, dx = pl.pallas_call(
            put,
            out_shape=tuple(jax.ShapeDtypeStruct(shape, dtype) for shape, dtype in shapes),
            in_specs=[any_spec] * 3,
            out_specs=(any_spec,) * 3,
            scratch_shapes=[dma((9,))],
            compiler_params=pltpu.CompilerParams(vmem_limit_bytes=1024 * 1024),
        )(*outs)
        return r1[None, None], r2[None, None], dx[None]

    spec_row = P(('grp', 'pp'), 'dp', None)
    spec_saved = P(('grp', 'pp'), None, None, 'dp', None)
    spec_w = P(('grp', 'pp'), None, None, None)
    spec_acc = P(('grp', 'pp'), 'dp', None, None, None)
    spec_g = P(('grp', 'pp'), None, 'dp', None)
    return jax.shard_map(body, mesh=mesh, in_specs=(spec_row, spec_saved, spec_saved, spec_w, spec_w, spec_acc, spec_acc), out_specs=(spec_g, spec_g, spec_row), check_vma=False)
```

```python
import functools

import jax
import jax.numpy as jnp
from jax import lax
from jax.experimental import pallas as pl
from jax.experimental.pallas import tpu as pltpu
from jax.sharding import PartitionSpec as P

MESH = pl.DeviceIdType.MESH
EARLY = (3,)
VMEM_LIMIT = 53 * 1024 * 1024
NN = (((1,), (0,)), ((), ()))
NT = (((1,), (1,)), ((), ()))
SQRT_2_OVER_PI = 0.7978845608028654
BF16 = jnp.bfloat16
F32 = jnp.float32


def dot(a, b, dims):
    return lax.dot_general(a, b, dims, preferred_element_type=F32)


def kernel(npp, ndp, tok, nchunk, dy, xs, hs, w1, w2, acc1, acc2, g1, g2, dx,
           w1v, w2v, recv1, recv2, hv, xv, act, slope, dht, xt, gt, uacc, first, gin, gout, relay, ident,
           stage1, stage2, early_acc, early_act, early_g, dyv,
           ld_sem, h_sem, x_sem, w2_sem, w1_sem, st1_sem, st2_sem, hop_send, hop_recv,
           send1, recv1_sem, send2, recv2_sem, far_recv, unit_recv, relay_send, relay_recv,
           early_send, early_recv):
    s = lax.axis_index('pp')
    p = lax.axis_index('dp')
    dm, ff = w1v.shape
    blk = ident.shape[0]
    half = 2 * tok
    hb = blk // 2
    nw2 = w2_sem.shape[0]
    w2rows = ff // nw2
    nblk = dm // blk
    q1 = dm // ndp
    q2 = ff // ndp
    rc1, cc1 = stage1.shape[2:]
    rc, cc = first.shape[1:]
    halves = q1 // rc1
    across = dm // cc
    mrows = 1024
    ru = rc // 4
    shed = (5, 2)
    early = tuple(zip((nchunk - 1, nchunk - 2), EARLY))

    far = (p + 2) % ndp
    peer = (p, p + 1 - 2 * (p % 2), far, far + 1 - 2 * (far % 2))

    far_k = (2, 3)
    order = far_k + (1, 0)

    def w2_copy(i):
        rows = pl.ds(i * w2rows, w2rows)
        return pltpu.make_async_copy(w2.at[rows, :], w2v.at[rows, :], w2_sem.at[i])

    def w1_copy(i):
        rows = pl.ds(i * blk, blk)
        return pltpu.make_async_copy(w1.at[rows, :], w1v.at[rows, :], w1_sem.at[i])

    def rows1(i, k):
        return pl.ds(pl.multiple_of(peer[k] * q1 + (i % halves) * rc1, rc1), rc1)

    def cols1(i):
        return pl.ds(pl.multiple_of((i // halves) * cc1, cc1), cc1)

    def rows2(i, k):
        return pl.ds(pl.multiple_of(peer[k] * q2 + (i // across) * rc, rc), rc)

    def cols2(i):
        return pl.ds(pl.multiple_of((i % across) * cc, cc), cc)

    def acc1_copy(i, k):
        return pltpu.make_async_copy(acc1.at[rows1(i, k), cols1(i)], stage1.at[i % 2, k], st1_sem.at[i % 2])

    def acc1_wait(i):
        pltpu.make_async_copy(stage1.at[i % 2], stage1.at[i % 2], st1_sem.at[i % 2]).wait()

    def slot2(i, k, n=1):
        return pl.ds(pl.multiple_of(((i % 2) * ndp + k) * rc, rc), n * rc)

    def acc2_copy(i, k):
        return pltpu.make_async_copy(acc2.at[rows2(i, k), cols2(i)], slope.at[slot2(i, k), :], st2_sem.at[i % 2])

    def acc2_wait(i):
        span = slope.at[slot2(i, 0, ndp), :]
        pltpu.make_async_copy(span, span, st2_sem.at[i % 2]).wait()

    def first_copy(k):
        return pltpu.make_async_copy(acc2.at[rows2(0, k), cols2(0)], stage2.at[k], st2_sem.at[2])

    def h_copy(t):
        rows = pl.ds((npp - 1 - s - t) * tok, tok)
        return pltpu.make_async_copy(hs.at[rows, :], hv.at[pl.ds(t * tok, tok), :], h_sem.at[t])

    def x_copy(t):
        rows = pl.ds((npp - 1 - s - t) * tok, tok)
        return pltpu.make_async_copy(xs.at[rows, :], xv.at[pl.ds(t * tok, tok), :], x_sem.at[t])

    dy_copy = pltpu.make_async_copy(dy, dyv, ld_sem.at[0])

    def used(t, start):
        @pl.when(t < npp - s)
        def _():
            start(t)

    for t in range(2):
        used(t, lambda t: h_copy(t).start())
    dy_copy.start()
    for i in range(1):
        w2_copy(i).start()

    barrier = pltpu.get_barrier_semaphore()
    for k in range(1, ndp):
        pl.semaphore_signal(barrier, inc=1, device_id={'dp': peer[k]}, device_id_type=MESH)
    for k in range(1, npp):
        pl.semaphore_signal(barrier, inc=1, device_id={'pp': (s + k) % npp}, device_id_type=MESH)

    for k in far_k:
        pl.semaphore_signal(barrier, inc=1, device_id={'pp': npp - 1 - s, 'dp': peer[k]}, device_id_type=MESH)

    rid = lax.broadcasted_iota(jnp.int32, (blk, blk), 0)
    cid = lax.broadcasted_iota(jnp.int32, (blk, blk), 1)
    ident[...] = jnp.where(rid == cid, 1.0, 0.0).astype(BF16)
    low = lax.broadcasted_iota(jnp.int32, (hb, half), 1) < tok

    def h_wait(t):
        @pl.when(t < npp - s)
        def _():
            h_copy(t).wait()

        @pl.when(t >= npp - s)
        def _():
            hv[t * tok:(t + 1) * tok, :] = jnp.zeros((tok, ff), BF16)

    def gelu_block(i, lanes):
        rows = slice(i * blk, (i + 1) * blk) if isinstance(i, int) else pl.ds(pl.multiple_of(i * blk, blk), blk)
        h = dot(ident[...], hv[lanes, rows], NT)
        h2 = h * h
        t = jnp.tanh(h * (SQRT_2_OVER_PI + (SQRT_2_OVER_PI * 0.044715) * h2))
        cdf = 0.5 + 0.5 * t
        a = h * cdf
        act[rows, lanes] = a.astype(BF16)
        slope[rows, lanes] = cdf + (a * (1.0 - cdf)) * (2.0 * SQRT_2_OVER_PI + (6.0 * SQRT_2_OVER_PI * 0.044715) * h2)

    def gelu(hh, start, stop):
        def step(i, _):
            gelu_block(i, slice(hh * half, (hh + 1) * half))
            return 0

        with jax.named_scope('gelu'):
            lax.fori_loop(start, stop, step, 0, unroll=4)

    gt[...] = jnp.zeros_like(gt)

    @pl.when(s >= npp - 2)
    def _():
        early_act[:, half:] = jnp.zeros((rc, half), BF16)
        for n in range(len(early)):
            early_g[n, :, half:] = jnp.zeros((cc, half), BF16)

    for i in range(1, nw2):
        w2_copy(i).start()
    with jax.named_scope('hwait'):
        for t in range(2):
            h_wait(t)
        dy_copy.wait()
    for c in range(nblk):
        gt[c * blk:(c + 1) * blk, 0:tok] = dot(ident[...], dyv[:, c * blk:(c + 1) * blk], NT).astype(BF16)

    at0 = 1 - jnp.minimum(s, 1)

    def hop_copy(t, c):
        slot = t + (npp - 1 - t) * at0
        return pltpu.make_async_remote_copy(
            src_ref=gout.at[t, c], dst_ref=gin.at[slot, c], send_sem=hop_send.at[t], recv_sem=hop_recv.at[slot, c],
            device_id={'pp': (s - 1) * (1 - at0) + (npp - 1 - t) * at0}, device_id_type=MESH)

    def hop_wait(slot, c):
        pltpu.make_async_remote_copy(
            src_ref=gin.at[slot, c], dst_ref=gin.at[slot, c], send_sem=hop_send.at[0], recv_sem=hop_recv.at[slot, c],
            device_id={'pp': s}, device_id_type=MESH).wait_recv()

    slot_of = {1: 0, 3: 1, 2: 2}

    def sems2(i, k):
        return dict(send_sem=send2.at[1 if k == 2 else 0], recv_sem=far_recv.at[i] if k == 2 else recv2_sem.at[i],
                    device_id={'dp': peer[k]}, device_id_type=MESH)

    def send_first(k):
        return pltpu.make_async_remote_copy(src_ref=first.at[k], dst_ref=recv2.at[slot_of[k], 0], **sems2(0, k))

    hl = (slice(0, half), slice(half, 2 * half))

    def early_on(n):
        return s < early[n][1]

    def early_copy(what, n, hh, cond_start=True):
        i = early[n][0]
        if what == 'acc':
            src, dst, q = acc2.at[rows2(i, 2), cols2(i)], early_acc.at[n], n
        elif what == 'act':
            src, dst, q = act.at[rows2(i, 2), hl[hh]], early_act.at[:, hl[hh]], 2 + hh
        else:
            src, dst, q = gt.at[cols2(i), hl[hh]], early_g.at[n, :, hl[hh]], 4 + 2 * n + hh
        return pltpu.make_async_remote_copy(
            src_ref=src, dst_ref=dst, send_sem=early_send.at[q], recv_sem=early_recv.at[q],
            device_id={'dp': peer[2]}, device_id_type=MESH)

    def early_start():
        for n in range(len(early)):
            @pl.when(early_on(n))
            def _():
                early_copy('acc', n, 0).start()

    def early_gt(hh, cond=None):
        for n in range(len(early)):
            @pl.when(early_on(n) if cond is None else early_on(n) & cond)
            def _():
                early_copy('g', n, hh).start()


    def first_chunk():
        with jax.named_scope('first'):
            pltpu.make_async_copy(stage2, stage2, st2_sem.at[2]).wait()
            for k in order:
                first[k] = (stage2[k] + dot(act[rows2(0, k), :], gt[0:cc, :], NT)).astype(BF16)
                if k == order[1]:
                    send_first(order[0]).start()
                    send_first(order[1]).start()
            send_first(order[2]).start()

    def unpack(packed, c, t):
        lanes = slice((t // 2) * half, (t // 2 + 1) * half)
        v = packed.astype(F32)
        r = pltpu.roll(v, tok, 1)
        for b, (lo, hi) in enumerate(((v, r), (r, v))):
            rows = slice(c * blk + b * hb, c * blk + (b + 1) * hb)
            if t % 2 == 0:
                new = jnp.where(low, lo, 0.0)
            else:
                new = jnp.where(low, gt[rows, lanes].astype(F32), hi)
            gt[rows, lanes] = new.astype(BF16)

    for t in range(npp):
        lanes = slice((t // 2) * half, (t // 2 + 1) * half)

        @pl.when(t < npp - s)
        def _(t=t, lanes=lanes):
            if t == 0:
                gelu(0, 0, ff // blk // 2)
                with jax.named_scope('barrier'):
                    pl.semaphore_wait(barrier, ndp - 1 + npp - 1 + len(far_k))
                early_start()
                with jax.named_scope('u0'):
                    for part in range(2):
                        for b in range(nw2 // 2):
                            w2_copy(part * (nw2 // 2) + b).wait()
                        for i in range(nblk if part == 0 else 0):
                            w1_copy(i).start()
                        for c in range(nblk):
                            krows = slice(c * blk, (c + 1) * blk)
                            for i in range(ff // mrows // 2):
                                rows = slice(part * (ff // 2) + i * mrows, part * (ff // 2) + (i + 1) * mrows)
                                u = dot(w2v[rows, krows], gt[krows, lanes], NN)
                                if c > 0:
                                    u = uacc[rows, :] + u
                                if c < nblk - 1:
                                    uacc[rows, :] = u
                                else:
                                    dht[rows, lanes] = (slope[rows, lanes] * u).astype(BF16)
                                if part == 0:
                                    gelu_block(ff // blk // 2 + c * 2 + i, lanes)

                @pl.when(early_on(0))
                def _():
                    early_copy('act', 0, 0).start()
                for t2 in range(2, npp):
                    used(t2, lambda t2: h_copy(t2).start())
                for t2 in range(npp):
                    used(t2, lambda t2: x_copy(t2).start())
            else:
                groups = ((0,), (1,), (2,), (3,))
                for group in groups:
                    for c in group:
                        with jax.named_scope('gwait'):
                            hop_wait(t - 1, c)
                        unpack(gin[t - 1, c], c, t)
                    if group == groups[-1]:
                        if t == npp - 1:
                            first_chunk()
                            early_gt(1)
                        elif t == npp - 2:
                            early_gt(1, s == 1)
                        elif t == 1:
                            early_gt(0)
                    krows = slice(group[0] * blk, (group[-1] + 1) * blk)

                    with jax.named_scope('u'):
                        for i in range(ff // mrows):
                            rows = slice(i * mrows, (i + 1) * mrows)
                            u = dot(w2v[rows, krows], gt[krows, lanes], NN)
                            if group != groups[0]:
                                u = uacc[rows, :] + u
                            if group != groups[-1]:
                                uacc[rows, :] = u
                            else:
                                dht[rows, lanes] = (slope[rows, lanes] * u).astype(BF16)

            def gx_dot(c, part):
                rows = slice(c * blk, (c + 1) * blk)
                k = slice(part * (ff // 2), (part + 1) * (ff // 2))
                return dot(w1v[rows, k], dht[k, lanes], NN)

            def gx_put(c, z):
                top, bot = z[:hb], z[hb:]
                if t % 2 == 0:
                    z = jnp.where(low, top, pltpu.roll(bot, tok, 1))
                else:
                    z = jnp.where(low, pltpu.roll(top, tok, 1), bot)
                gout[t, c] = z.astype(BF16)

                if t < npp - 1:
                    hop_copy(t, c).start()

            with jax.named_scope('gx'):
                last = None
                for c in range(nblk):
                    if t == 0 and c % 2 == 0:
                        w1_copy(c).wait()
                        w1_copy(c + 1).wait()
                    if t == 0 and c == 0:
                        for k in range(ndp):
                            first_copy(k).start()
                        for i in range(2):
                            for k in range(ndp):
                                acc1_copy(i, k).start()
                    z = gt[c * blk:(c + 1) * blk, lanes].astype(F32) + gx_dot(c, 0)
                    if c > 0:
                        gx_put(c - 1, last)
                    last = z + gx_dot(c, 1)
                gx_put(nblk - 1, last)

        if t == 0:
            @pl.when(s < npp - 2)
            def _():
                for t in range(2, npp):
                    h_wait(t)
                gelu(1, 0, ff // blk)

                @pl.when(early_on(0))
                def _():
                    early_copy('act', 0, 1).start()

            @pl.when(s >= npp - 2)
            def _():
                act[:, half:] = jnp.zeros((ff, half), BF16)
                dht[:, half:] = jnp.zeros((ff, half), BF16)

    for i in range(1, 3):
        for k in range(ndp):
            acc2_copy(i, k).start()

    @pl.when(s > 0)
    def _():
        first_chunk()

    for t in range(npp):
        @pl.when(t < npp - s)
        def _():
            x_copy(t).wait()

        @pl.when(t >= npp - s)
        def _():
            xv[t * tok:(t + 1) * tok, :] = jnp.zeros((tok, dm), BF16)
    for c in range(nblk):
        rows = pl.ds(c * blk, blk)
        xt[rows, :] = dot(ident[...], xv[:, rows], NT).astype(BF16)

    def send2_copy(i, k):
        return pltpu.make_async_remote_copy(
            src_ref=w2v.at[rows2(i, k), cols2(i)], dst_ref=recv2.at[slot_of[k], i], **sems2(i, k))

    def send1_copy(i, k):
        return pltpu.make_async_remote_copy(
            src_ref=w1v.at[rows1(i, k), cols1(i)], dst_ref=recv1.at[i, k - 1],
            send_sem=send1.at[0], recv_sem=recv1_sem.at[i], device_id={'dp': peer[k]}, device_id_type=MESH)

    units = tuple((u, far_k[u // 4], u % 4) for u in range(8))

    def is_shed(u, stage):
        cond = jnp.bool_(False)
        for n, count in enumerate(shed):
            if u < count:
                cond = cond | (stage == n)
        return cond

    def unit_dst(k, b):
        return recv2.at[slot_of[k], 1, pl.ds(b * ru, ru), :]

    def unit_src(k, b):
        return w2v.at[pl.ds(pl.multiple_of(peer[k] * q2 + b * ru, ru), ru), cols2(1)]

    def unit_copy(u, k, b):
        return pltpu.make_async_remote_copy(
            src_ref=unit_src(k, b), dst_ref=unit_dst(k, b), send_sem=send2.at[1 if k == 2 else 0], recv_sem=unit_recv.at[u],
            device_id={'dp': peer[k]}, device_id_type=MESH)

    def shed_copy(u, k, b):
        return pltpu.make_async_remote_copy(
            src_ref=unit_src(k, b), dst_ref=relay.at[u], send_sem=send2.at[1 if k == 2 else 0], recv_sem=relay_recv.at[u],
            device_id={'pp': npp - 1 - s, 'dp': peer[k]}, device_id_type=MESH)

    def relay_copy(u, k, b):
        return pltpu.make_async_remote_copy(
            src_ref=relay.at[u], dst_ref=unit_dst(k, b), send_sem=relay_send.at[u], recv_sem=unit_recv.at[u],
            device_id={'pp': npp - 1 - s}, device_id_type=MESH)

    def send_unit(u, k, b):
        cond = is_shed(u, s)

        @pl.when(cond)
        def _():
            shed_copy(u, k, b).start()

        @pl.when(jnp.logical_not(cond))
        def _():
            unit_copy(u, k, b).start()

    def a2_add(i):
        acc2_wait(i)
        for k in order:
            w2v[rows2(i, k), cols2(i)] = (
                slope[slot2(i, k), :] + dot(act[rows2(i, k), :], gt[cols2(i), :], NT)).astype(BF16)

    def a2_next(i):
        @pl.when(i + 2 < nchunk)
        def _():
            for k in range(ndp):
                acc2_copy(i + 2, k).start()

    plain = nchunk - len(early)

    def a2_step(i, _):
        a2_add(i)
        for k in order[:-1]:
            send2_copy(i, k).start()
        a2_next(i)
        return 0

    def far_copy(n):
        i = early[n][0]
        return pltpu.make_async_remote_copy(
            src_ref=w2v.at[rows2(i, 2), cols2(i)], dst_ref=recv2.at[slot_of[2], i],
            send_sem=send2.at[2 + n], recv_sem=far_recv.at[i], device_id={'dp': peer[2]}, device_id_type=MESH)

    with jax.named_scope('a2'):
        a2_add(1)
        for unit in units:
            send_unit(*unit)
        send2_copy(1, 1).start()
        a2_next(jnp.int32(1))
        lax.fori_loop(2, plain, a2_step, 0)
        for n in reversed(range(len(early))):
            i = early[n][0]
            a2_add(i)

            @pl.when(jnp.logical_not(early_on(n)))
            def _():
                far_copy(n).start()
            for k in (3, 1):
                send2_copy(i, k).start()

    with jax.named_scope('relay'):
        for u, k, b in units:
            @pl.when(is_shed(u, npp - 1 - s))
            def _():
                pltpu.make_async_remote_copy(
                    src_ref=relay.at[u], dst_ref=relay.at[u], send_sem=relay_send.at[u], recv_sem=relay_recv.at[u],
                    device_id={'pp': npp - 1 - s}, device_id_type=MESH).wait_recv()
                relay_copy(u, k, b).start()

    def a1_step(i, _):
        acc1_wait(i)
        for k in order:
            w1v[rows1(i, k), cols1(i)] = (
                stage1[i % 2, k] + dot(xt[rows1(i, k), :], dht[cols1(i), :], NT)).astype(BF16)
        for k in order[:-1]:
            send1_copy(i, k).start()

        @pl.when(i + 2 < nchunk)
        def _():
            for k in range(ndp):
                acc1_copy(i + 2, k).start()
        return 0

    with jax.named_scope('a1'):
        lax.fori_loop(0, nchunk, a1_step, 0)

    def put_dx(packed, c, e):
        v = packed.astype(F32)
        r = pltpu.roll(v, tok, 1)
        col = jnp.concatenate([v, r], axis=0).astype(BF16)
        dx[:, c * blk:(c + 1) * blk] = dot(ident[:tok, :half], col, NT).astype(BF16)

    for c in range(nblk):
        @pl.when(s == 0)
        def _():
            put_dx(gout[npp - 1, c], c, 0)

        @pl.when(s > 0)
        def _():
            hop_wait(npp - 1, c)
            put_dx(gin[npp - 1, c], c, 0)

    scale = 1.0 / ndp

    def all_of(ref, sem):
        return pltpu.make_async_copy(ref, ref, sem)

    def r2_sum(i, own):
        for k in range(1, ndp):
            own = own + recv2[slot_of[k], i].astype(F32)
        rows = pl.ds(pl.multiple_of((i // across) * rc, rc), rc)
        g2[rows, cols2(i)] = own * scale

    def r2_wait(i):
        with jax.named_scope('r2wait'):
            all_of(recv2.at[0:2, i], recv2_sem.at[i]).wait()
            all_of(recv2.at[2, i], far_recv.at[i]).wait()

    r2_wait(0)
    r2_sum(0, first[0].astype(F32))

    for u, k, b in units:
        all_of(relay.at[u], unit_recv.at[u]).wait()
    all_of(recv2.at[0, 1], recv2_sem.at[1]).wait()
    r2_sum(1, w2v[rows2(1, 0), cols2(1)].astype(F32))

    def r2_step(i, _):
        r2_wait(i)
        r2_sum(i, w2v[rows2(i, 0), cols2(i)].astype(F32))
        return 0

    lax.fori_loop(2, plain, r2_step, 0)

    for n in reversed(range(len(early))):
        i = early[n][0]

        @pl.when(early_on(n))
        def _():
            early_copy('acc', n, 0).wait()
            for hh in range(2):
                if hh == 0:
                    if n == 0:
                        early_copy('act', n, hh).wait()
                    early_copy('g', n, hh).wait()
                else:
                    @pl.when(s < npp - 2)
                    def _():
                        if n == 0:
                            early_copy('act', n, hh).wait()
                        early_copy('g', n, hh).wait()
            recv2[slot_of[2], i] = (early_acc[n] + dot(early_act[...], early_g[n], NT)).astype(BF16)

        @pl.when(jnp.logical_not(early_on(n)))
        def _():
            far_copy(n).wait()
        with jax.named_scope('r2wait'):
            all_of(recv2.at[0:2, i], recv2_sem.at[i]).wait()
        r2_sum(i, w2v[rows2(i, 0), cols2(i)].astype(F32))

    def r1_step(i, _):
        with jax.named_scope('r1wait'):
            all_of(recv1.at[i], recv1_sem.at[i]).wait()
        with jax.named_scope('r1sum'):
            tot = w1v[rows1(i, 0), cols1(i)].astype(F32)
            for k in range(1, ndp):
                tot = tot + recv1[i, k - 1].astype(F32)
            g1[pl.ds(pl.multiple_of((i % halves) * rc1, rc1), rc1), cols1(i)] = tot * scale
        return 0

    lax.fori_loop(0, nchunk, r1_step, 0)

    with jax.named_scope('tail'):
        all_of(recv1, send1.at[0]).wait()
        all_of(recv2.at[0:2], send2.at[0]).wait()
        all_of(recv2.at[2, 0:plain], send2.at[1]).wait()
        for u, k, b in units:
            @pl.when(is_shed(u, npp - 1 - s))
            def _():
                relay_copy(u, k, b).wait_send()
        for t in range(npp - 1):
            @pl.when(t < npp - s)
            def _():
                all_of(gout.at[t], hop_send.at[t]).wait()


def put(g1, g2, dx, o1, o2, o3, sems):
    pieces = 4
    copies = []
    for n, (src, dst) in enumerate(((g1, o1), (g2, o2))):
        size = src.shape[0] // pieces
        for i in range(pieces):
            rows = pl.ds(i * size, size)
            copies.append(pltpu.make_async_copy(src.at[rows, :], dst.at[rows, :], sems.at[n * pieces + i]))
    copies.append(pltpu.make_async_copy(dx, o3, sems.at[2 * pieces]))
    for copy in copies:
        copy.start()
    for copy in copies:
        copy.wait()


def solution(mesh):
    npp = mesh.shape['pp']
    ndp = mesh.shape['dp']

    def body(dy, xs, hs, w1, w2, acc1, acc2):
        tok = dy.shape[1]
        dm, ff = w1.shape[2:]
        ntok = npp * tok
        nchunk = 8
        blk = 256
        nblk = dm // blk
        q1, q2 = dm // ndp, ff // ndp
        rc1, cc1 = q1 // 2, ff // (nchunk // 2)
        rc, cc = q2 // 2, dm // (nchunk // 2)
        dma = pltpu.SemaphoreType.DMA
        any_spec = pl.BlockSpec(memory_space=pl.ANY)
        vmem = pl.BlockSpec(memory_space=pltpu.VMEM)
        shapes = ((q1, ff), F32), ((q2, dm), F32), ((tok, dm), BF16)
        outs = pl.pallas_call(
            functools.partial(kernel, npp, ndp, tok, nchunk),
            out_shape=tuple(pltpu.VMEM(shape, dtype) for shape, dtype in shapes),
            in_specs=[any_spec] * 7,
            out_specs=(vmem,) * 3,
            scratch_shapes=[
                pltpu.VMEM((dm, ff), BF16), pltpu.VMEM((ff, dm), BF16),
                pltpu.VMEM((nchunk, ndp - 1, rc1, cc1), BF16), pltpu.VMEM((ndp - 1, nchunk, rc, cc), BF16),
                pltpu.VMEM((ntok, ff), BF16), pltpu.VMEM((ntok, dm), BF16),
                pltpu.VMEM((ff, ntok), BF16), pltpu.VMEM((ff, ntok), F32), pltpu.VMEM((ff, ntok), BF16),
                pltpu.VMEM((dm, ntok), BF16), pltpu.VMEM((dm, ntok), BF16), pltpu.VMEM((ff, 2 * tok), F32),
                pltpu.VMEM((ndp, rc, cc), BF16),
                pltpu.VMEM((npp, nblk, blk // 2, 2 * tok), BF16), pltpu.VMEM((npp, nblk, blk // 2, 2 * tok), BF16),
                pltpu.VMEM((8, rc // 4, cc), BF16), pltpu.VMEM((blk, blk), BF16),
                pltpu.VMEM((2, ndp, rc1, cc1), F32), pltpu.VMEM((ndp, rc, cc), F32),
                pltpu.VMEM((len(EARLY), rc, cc), F32), pltpu.VMEM((rc, ntok), BF16), pltpu.VMEM((len(EARLY), cc, ntok), BF16),
                pltpu.VMEM((tok, dm), BF16),
                dma((1,)), dma((npp,)), dma((npp,)), dma((8,)), dma((nblk,)), dma((2,)), dma((3,)),
                dma((npp - 1,)), dma((npp, nblk)),
                dma((1,)), dma((nchunk,)), dma((4,)), dma((nchunk,)), dma((nchunk,)), dma((8,)), dma((8,)), dma((8,)),
                dma((8,)), dma((8,)),
            ],
            compiler_params=pltpu.CompilerParams(
                collective_id=0, has_side_effects=True, vmem_limit_bytes=VMEM_LIMIT),
        )(dy[0], xs.reshape(ntok, dm), hs.reshape(ntok, ff), w1[0, 0], w2[0, 0], acc1[0, 0, 0], acc2[0, 0, 0])
        r1, r2, dx = pl.pallas_call(
            put,
            out_shape=tuple(jax.ShapeDtypeStruct(shape, dtype) for shape, dtype in shapes),
            in_specs=[any_spec] * 3,
            out_specs=(any_spec,) * 3,
            scratch_shapes=[dma((9,))],
            compiler_params=pltpu.CompilerParams(vmem_limit_bytes=1024 * 1024),
        )(*outs)
        return r1[None, None], r2[None, None], dx[None]

    spec_row = P(('grp', 'pp'), 'dp', None)
    spec_saved = P(('grp', 'pp'), None, None, 'dp', None)
    spec_w = P(('grp', 'pp'), None, None, None)
    spec_acc = P(('grp', 'pp'), 'dp', None, None, None)
    spec_g = P(('grp', 'pp'), None, 'dp', None)
    return jax.shard_map(body, mesh=mesh, in_specs=(spec_row, spec_saved, spec_saved, spec_w, spec_w, spec_acc, spec_acc), out_specs=(spec_g, spec_g, spec_row), check_vma=False)
```

```python
import functools

import jax
import jax.numpy as jnp
from jax import lax
from jax.experimental import pallas as pl
from jax.experimental.pallas import tpu as pltpu
from jax.sharding import PartitionSpec as P

MESH = pl.DeviceIdType.MESH
EARLY = (3,)
VMEM_LIMIT = 53 * 1024 * 1024
NN = (((1,), (0,)), ((), ()))
NT = (((1,), (1,)), ((), ()))
SQRT_2_OVER_PI = 0.7978845608028654
BF16 = jnp.bfloat16
F32 = jnp.float32


def dot(a, b, dims):
    return lax.dot_general(a, b, dims, preferred_element_type=F32)


def kernel(npp, ndp, tok, nchunk, dy, xs, hs, w1, w2, acc1, acc2, g1, g2, dx,
           w1v, w2v, recv1, recv2, hv, xv, act, slope, dht, xt, gt, uacc, first, gin, gout, relay, ident,
           stage1, stage2, early_acc, early_act, early_g, dyv,
           ld_sem, h_sem, x_sem, w2_sem, w1_sem, st1_sem, st2_sem, hop_send, hop_recv,
           send1, recv1_sem, send2, recv2_sem, far_recv, unit_recv, relay_send, relay_recv,
           early_send, early_recv):
    s = lax.axis_index('pp')
    p = lax.axis_index('dp')
    dm, ff = w1v.shape
    blk = ident.shape[0]
    half = 2 * tok
    hb = blk // 2
    nw2 = w2_sem.shape[0]
    w2rows = ff // nw2
    nblk = dm // blk
    q1 = dm // ndp
    q2 = ff // ndp
    rc1, cc1 = stage1.shape[2:]
    rc, cc = first.shape[1:]
    halves = q1 // rc1
    across = dm // cc
    mrows = 1024
    shed = (6, 2)
    early = tuple(zip((nchunk - 1, nchunk - 2), EARLY))

    far = (p + 2) % ndp
    peer = (p, p + 1 - 2 * (p % 2), far, far + 1 - 2 * (far % 2))

    far_k = (2, 3)
    order = far_k + (1, 0)

    def w2_copy(i):
        rows = pl.ds(i * w2rows, w2rows)
        return pltpu.make_async_copy(w2.at[rows, :], w2v.at[rows, :], w2_sem.at[i])

    def w1_copy(i):
        rows = pl.ds(i * blk, blk)
        return pltpu.make_async_copy(w1.at[rows, :], w1v.at[rows, :], w1_sem.at[i])

    def rows1(i, k):
        return pl.ds(pl.multiple_of(peer[k] * q1 + (i % halves) * rc1, rc1), rc1)

    def cols1(i):
        return pl.ds(pl.multiple_of((i // halves) * cc1, cc1), cc1)

    def rows2(i, k):
        return pl.ds(pl.multiple_of(peer[k] * q2 + (i // across) * rc, rc), rc)

    def cols2(i):
        return pl.ds(pl.multiple_of((i % across) * cc, cc), cc)

    def acc1_copy(i, k):
        return pltpu.make_async_copy(acc1.at[rows1(i, k), cols1(i)], stage1.at[i % 2, k], st1_sem.at[i % 2])

    def acc1_wait(i):
        pltpu.make_async_copy(stage1.at[i % 2], stage1.at[i % 2], st1_sem.at[i % 2]).wait()

    def slot2(i, k, n=1):
        return pl.ds(pl.multiple_of(((i % 2) * ndp + k) * rc, rc), n * rc)

    def acc2_copy(i, k):
        return pltpu.make_async_copy(acc2.at[rows2(i, k), cols2(i)], slope.at[slot2(i, k), :], st2_sem.at[i % 2])

    def acc2_wait(i):
        span = slope.at[slot2(i, 0, ndp), :]
        pltpu.make_async_copy(span, span, st2_sem.at[i % 2]).wait()

    def first_copy(k):
        return pltpu.make_async_copy(acc2.at[rows2(0, k), cols2(0)], stage2.at[k], st2_sem.at[2])

    def h_copy(t):
        rows = pl.ds((npp - 1 - s - t) * tok, tok)
        return pltpu.make_async_copy(hs.at[rows, :], hv.at[pl.ds(t * tok, tok), :], h_sem.at[t])

    def x_copy(t):
        rows = pl.ds((npp - 1 - s - t) * tok, tok)
        return pltpu.make_async_copy(xs.at[rows, :], xv.at[pl.ds(t * tok, tok), :], x_sem.at[t])

    dy_copy = pltpu.make_async_copy(dy, dyv, ld_sem.at[0])

    def used(t, start):
        @pl.when(t < npp - s)
        def _():
            start(t)

    for t in range(2):
        used(t, lambda t: h_copy(t).start())
    dy_copy.start()
    for i in range(1):
        w2_copy(i).start()

    barrier = pltpu.get_barrier_semaphore()
    for k in range(1, ndp):
        pl.semaphore_signal(barrier, inc=1, device_id={'dp': peer[k]}, device_id_type=MESH)
    for k in range(1, npp):
        pl.semaphore_signal(barrier, inc=1, device_id={'pp': (s + k) % npp}, device_id_type=MESH)

    for k in far_k:
        pl.semaphore_signal(barrier, inc=1, device_id={'pp': npp - 1 - s, 'dp': peer[k]}, device_id_type=MESH)

    rid = lax.broadcasted_iota(jnp.int32, (blk, blk), 0)
    cid = lax.broadcasted_iota(jnp.int32, (blk, blk), 1)
    ident[...] = jnp.where(rid == cid, 1.0, 0.0).astype(BF16)
    low = lax.broadcasted_iota(jnp.int32, (hb, half), 1) < tok

    def h_wait(t):
        @pl.when(t < npp - s)
        def _():
            h_copy(t).wait()

        @pl.when(t >= npp - s)
        def _():
            hv[t * tok:(t + 1) * tok, :] = jnp.zeros((tok, ff), BF16)

    def gelu_block(i, lanes):
        rows = slice(i * blk, (i + 1) * blk) if isinstance(i, int) else pl.ds(pl.multiple_of(i * blk, blk), blk)
        h = dot(ident[...], hv[lanes, rows], NT)
        h2 = h * h
        t = jnp.tanh(h * (SQRT_2_OVER_PI + (SQRT_2_OVER_PI * 0.044715) * h2))
        cdf = 0.5 + 0.5 * t
        a = h * cdf
        act[rows, lanes] = a.astype(BF16)
        slope[rows, lanes] = cdf + (a * (1.0 - cdf)) * (2.0 * SQRT_2_OVER_PI + (6.0 * SQRT_2_OVER_PI * 0.044715) * h2)

    def gelu(hh, start, stop):
        def step(i, _):
            gelu_block(i, slice(hh * half, (hh + 1) * half))
            return 0

        with jax.named_scope('gelu'):
            lax.fori_loop(start, stop, step, 0, unroll=4)

    gt[...] = jnp.zeros_like(gt)

    @pl.when(s >= npp - 2)
    def _():
        act[:, half:] = jnp.zeros((ff, half), BF16)
        dht[:, half:] = jnp.zeros((ff, half), BF16)
        early_act[:, half:] = jnp.zeros((rc, half), BF16)
        for n in range(len(early)):
            early_g[n, :, half:] = jnp.zeros((cc, half), BF16)

    for i in range(1, nw2):
        w2_copy(i).start()
    with jax.named_scope('hwait'):
        for t in range(2):
            h_wait(t)
        dy_copy.wait()
    for c in range(nblk):
        gt[c * blk:(c + 1) * blk, 0:tok] = dot(ident[...], dyv[:, c * blk:(c + 1) * blk], NT).astype(BF16)

    at0 = 1 - jnp.minimum(s, 1)

    def hop_copy(t, c):
        slot = t + (npp - 1 - t) * at0
        return pltpu.make_async_remote_copy(
            src_ref=gout.at[t, c], dst_ref=gin.at[slot, c], send_sem=hop_send.at[t], recv_sem=hop_recv.at[slot, c],
            device_id={'pp': (s - 1) * (1 - at0) + (npp - 1 - t) * at0}, device_id_type=MESH)

    def hop_wait(slot, c):
        pltpu.make_async_remote_copy(
            src_ref=gin.at[slot, c], dst_ref=gin.at[slot, c], send_sem=hop_send.at[0], recv_sem=hop_recv.at[slot, c],
            device_id={'pp': s}, device_id_type=MESH).wait_recv()

    slot_of = {1: 0, 3: 1, 2: 2}

    def sems2(i, k):
        return dict(send_sem=send2.at[1 if k == 2 else 0], recv_sem=far_recv.at[i] if k == 2 else recv2_sem.at[i],
                    device_id={'dp': peer[k]}, device_id_type=MESH)

    def send_first(k):
        return pltpu.make_async_remote_copy(src_ref=first.at[k], dst_ref=recv2.at[slot_of[k], 0], **sems2(0, k))

    hl = (slice(0, half), slice(half, 2 * half))

    def early_on(n):
        return s < early[n][1]

    def early_copy(what, n, hh, cond_start=True):
        i = early[n][0]
        if what == 'acc':
            src, dst, q = acc2.at[rows2(i, 2), cols2(i)], early_acc.at[n], n
        elif what == 'act':
            src, dst, q = act.at[rows2(i, 2), hl[hh]], early_act.at[:, hl[hh]], 2 + hh
        else:
            src, dst, q = gt.at[cols2(i), hl[hh]], early_g.at[n, :, hl[hh]], 4 + 2 * n + hh
        return pltpu.make_async_remote_copy(
            src_ref=src, dst_ref=dst, send_sem=early_send.at[q], recv_sem=early_recv.at[q],
            device_id={'dp': peer[2]}, device_id_type=MESH)

    def early_start():
        for n in range(len(early)):
            @pl.when(early_on(n))
            def _():
                early_copy('acc', n, 0).start()

    def early_gt(hh, cond=None):
        for n in range(len(early)):
            @pl.when(early_on(n) if cond is None else early_on(n) & cond)
            def _():
                early_copy('g', n, hh).start()


    def first_chunk():
        with jax.named_scope('first'):
            pltpu.make_async_copy(stage2, stage2, st2_sem.at[2]).wait()
            for k in order:
                first[k] = (stage2[k] + dot(act[rows2(0, k), :], gt[0:cc, :], NT)).astype(BF16)
                if k == order[1]:
                    send_first(order[0]).start()
                    send_first(order[1]).start()
            send_first(order[2]).start()

    def unpack(packed, c, t):
        lanes = slice((t // 2) * half, (t // 2 + 1) * half)
        v = packed.astype(F32)
        r = pltpu.roll(v, tok, 1)
        for b, (lo, hi) in enumerate(((v, r), (r, v))):
            rows = slice(c * blk + b * hb, c * blk + (b + 1) * hb)
            if t % 2 == 0:
                new = jnp.where(low, lo, 0.0)
            else:
                new = jnp.where(low, gt[rows, lanes].astype(F32), hi)
            gt[rows, lanes] = new.astype(BF16)

    for t in range(npp):
        lanes = slice((t // 2) * half, (t // 2 + 1) * half)

        @pl.when(t < npp - s)
        def _(t=t, lanes=lanes):
            if t == 0:
                gelu(0, 0, ff // blk // 2)
                with jax.named_scope('barrier'):
                    pl.semaphore_wait(barrier, ndp - 1 + npp - 1 + len(far_k))
                early_start()
                with jax.named_scope('u0'):
                    for part in range(2):
                        for b in range(nw2 // 2):
                            w2_copy(part * (nw2 // 2) + b).wait()
                        if part == 0:
                            @pl.when(s == npp - 1)
                            def _():
                                for k in range(ndp):
                                    first_copy(k).start()
                            for i in range(nblk):
                                w1_copy(i).start()
                        for c in range(nblk):
                            krows = slice(c * blk, (c + 1) * blk)
                            for i in range(ff // mrows // 2):
                                rows = slice(part * (ff // 2) + i * mrows, part * (ff // 2) + (i + 1) * mrows)
                                u = dot(w2v[rows, krows], gt[krows, lanes], NN)
                                if c > 0:
                                    u = uacc[rows, :] + u
                                if c < nblk - 1:
                                    uacc[rows, :] = u
                                else:
                                    dht[rows, lanes] = (slope[rows, lanes] * u).astype(BF16)
                                if part == 0:
                                    gelu_block(ff // blk // 2 + c * 2 + i, lanes)

                @pl.when(early_on(0))
                def _():
                    early_copy('act', 0, 0).start()
                for t2 in range(2, npp):
                    used(t2, lambda t2: h_copy(t2).start())
                for t2 in range(npp):
                    used(t2, lambda t2: x_copy(t2).start())
            else:
                groups = ((0,), (1,), (2,), (3,))
                for group in groups:
                    for c in group:
                        with jax.named_scope('gwait'):
                            hop_wait(t - 1, c)
                        unpack(gin[t - 1, c], c, t)
                    if group == groups[-1]:
                        if t == npp - 1:
                            first_chunk()
                            early_gt(1)
                        elif t == npp - 2:
                            early_gt(1, s == 1)
                        elif t == 1:
                            early_gt(0)
                    krows = slice(group[0] * blk, (group[-1] + 1) * blk)

                    with jax.named_scope('u'):
                        for i in range(ff // mrows):
                            rows = slice(i * mrows, (i + 1) * mrows)
                            u = dot(w2v[rows, krows], gt[krows, lanes], NN)
                            if group != groups[0]:
                                u = uacc[rows, :] + u
                            if group != groups[-1]:
                                uacc[rows, :] = u
                            else:
                                dht[rows, lanes] = (slope[rows, lanes] * u).astype(BF16)

            def gx_dot(c, part):
                rows = slice(c * blk, (c + 1) * blk)
                k = slice(part * (ff // 2), (part + 1) * (ff // 2))
                return dot(w1v[rows, k], dht[k, lanes], NN)

            def gx_put(c, z):
                top, bot = z[:hb], z[hb:]
                if t % 2 == 0:
                    z = jnp.where(low, top, pltpu.roll(bot, tok, 1))
                else:
                    z = jnp.where(low, pltpu.roll(top, tok, 1), bot)
                gout[t, c] = z.astype(BF16)

                if t < npp - 1:
                    hop_copy(t, c).start()

            with jax.named_scope('gx'):
                last = None
                for c in range(nblk):
                    if t == 0 and c % 2 == 0:
                        w1_copy(c).wait()
                        w1_copy(c + 1).wait()
                    if t == 0 and c == 0:
                        @pl.when(s < npp - 1)
                        def _():
                            for k in range(ndp):
                                first_copy(k).start()
                        for i in range(2):
                            for k in range(ndp):
                                acc1_copy(i, k).start()
                    if t == 0 and c == 2:
                        gx_put(1, last)

                        @pl.when(s == npp - 1)
                        def _():
                            first_chunk()
                    z = gt[c * blk:(c + 1) * blk, lanes].astype(F32) + gx_dot(c, 0)
                    if c > 0 and not (t == 0 and c == 2):
                        gx_put(c - 1, last)
                    last = z + gx_dot(c, 1)
                gx_put(nblk - 1, last)

        if t == 0:
            @pl.when(s < npp - 2)
            def _():
                for t in range(2, npp):
                    h_wait(t)
                gelu(1, 0, ff // blk)

                @pl.when(early_on(0))
                def _():
                    early_copy('act', 0, 1).start()

    for i in range(1, 3):
        for k in range(ndp):
            acc2_copy(i, k).start()

    @pl.when((s > 0) & (s < npp - 1))
    def _():
        first_chunk()

    for t in range(npp):
        @pl.when(t < npp - s)
        def _():
            x_copy(t).wait()

        @pl.when(t >= npp - s)
        def _():
            xv[t * tok:(t + 1) * tok, :] = jnp.zeros((tok, dm), BF16)
    for c in range(nblk):
        rows = pl.ds(c * blk, blk)
        xt[rows, :] = dot(ident[...], xv[:, rows], NT).astype(BF16)

    def send2_copy(i, k):
        return pltpu.make_async_remote_copy(
            src_ref=w2v.at[rows2(i, k), cols2(i)], dst_ref=recv2.at[slot_of[k], i], **sems2(i, k))

    def send1_copy(i, k):
        return pltpu.make_async_remote_copy(
            src_ref=w1v.at[rows1(i, k), cols1(i)], dst_ref=recv1.at[i, k - 1],
            send_sem=send1.at[0], recv_sem=recv1_sem.at[i], device_id={'dp': peer[k]}, device_id_type=MESH)

    pieces = ((0, rc // 4), (rc // 4, rc // 8), (3 * rc // 8, rc // 8), (rc // 2, rc // 2))
    units = tuple((u, far_k[u // 4], pieces[u % 4]) for u in range(8))

    def is_shed(u, stage):
        cond = jnp.bool_(False)
        for n, count in enumerate(shed):
            if u < count:
                cond = cond | (stage == n)
        return cond

    def unit_dst(k, b):
        return recv2.at[slot_of[k], 1, pl.ds(*b), :]

    def unit_src(k, b):
        return w2v.at[pl.ds(pl.multiple_of(peer[k] * q2 + b[0], rc // 8), b[1]), cols2(1)]

    def relay_at(k, b):
        return relay.at[far_k.index(k), pl.ds(*b), :]

    def unit_copy(u, k, b):
        return pltpu.make_async_remote_copy(
            src_ref=unit_src(k, b), dst_ref=unit_dst(k, b), send_sem=send2.at[1 if k == 2 else 0], recv_sem=unit_recv.at[u],
            device_id={'dp': peer[k]}, device_id_type=MESH)

    def shed_copy(u, k, b):
        return pltpu.make_async_remote_copy(
            src_ref=unit_src(k, b), dst_ref=relay_at(k, b), send_sem=send2.at[1 if k == 2 else 0], recv_sem=relay_recv.at[u],
            device_id={'pp': npp - 1 - s, 'dp': peer[k]}, device_id_type=MESH)

    def relay_copy(u, k, b):
        return pltpu.make_async_remote_copy(
            src_ref=relay_at(k, b), dst_ref=unit_dst(k, b), send_sem=relay_send.at[u], recv_sem=unit_recv.at[u],
            device_id={'pp': npp - 1 - s}, device_id_type=MESH)

    def send_unit(u, k, b):
        cond = is_shed(u, s)

        @pl.when(cond)
        def _():
            shed_copy(u, k, b).start()

        @pl.when(jnp.logical_not(cond))
        def _():
            unit_copy(u, k, b).start()

    def a2_add(i):
        acc2_wait(i)
        for k in order:
            w2v[rows2(i, k), cols2(i)] = (
                slope[slot2(i, k), :] + dot(act[rows2(i, k), :], gt[cols2(i), :], NT)).astype(BF16)

    def a2_next(i):
        @pl.when(i + 2 < nchunk)
        def _():
            for k in range(ndp):
                acc2_copy(i + 2, k).start()

    plain = nchunk - len(early)

    def a2_step(i, _):
        a2_add(i)
        for k in order[:-1]:
            send2_copy(i, k).start()
        a2_next(i)
        return 0

    def far_copy(n):
        i = early[n][0]
        return pltpu.make_async_remote_copy(
            src_ref=w2v.at[rows2(i, 2), cols2(i)], dst_ref=recv2.at[slot_of[2], i],
            send_sem=send2.at[2 + n], recv_sem=far_recv.at[i], device_id={'dp': peer[2]}, device_id_type=MESH)

    with jax.named_scope('a2'):
        a2_add(1)
        for unit in units:
            send_unit(*unit)
        send2_copy(1, 1).start()
        a2_next(jnp.int32(1))
        lax.fori_loop(2, plain, a2_step, 0)
        for n in reversed(range(len(early))):
            i = early[n][0]
            a2_add(i)

            @pl.when(jnp.logical_not(early_on(n)))
            def _():
                far_copy(n).start()
            for k in (3, 1):
                send2_copy(i, k).start()

    with jax.named_scope('relay'):
        for u, k, b in units:
            @pl.when(is_shed(u, npp - 1 - s))
            def _():
                pltpu.make_async_remote_copy(
                    src_ref=relay_at(k, b), dst_ref=relay_at(k, b), send_sem=relay_send.at[u], recv_sem=relay_recv.at[u],
                    device_id={'pp': npp - 1 - s}, device_id_type=MESH).wait_recv()
                relay_copy(u, k, b).start()

    def a1_step(i, _):
        acc1_wait(i)
        for k in order:
            w1v[rows1(i, k), cols1(i)] = (
                stage1[i % 2, k] + dot(xt[rows1(i, k), :], dht[cols1(i), :], NT)).astype(BF16)
        for k in order[:-1]:
            send1_copy(i, k).start()

        @pl.when(i + 2 < nchunk)
        def _():
            for k in range(ndp):
                acc1_copy(i + 2, k).start()
        return 0

    with jax.named_scope('a1'):
        lax.fori_loop(0, nchunk, a1_step, 0)

    def put_dx(packed, c, e):
        v = packed.astype(F32)
        r = pltpu.roll(v, tok, 1)
        col = jnp.concatenate([v, r], axis=0).astype(BF16)
        dx[:, c * blk:(c + 1) * blk] = dot(ident[:tok, :half], col, NT).astype(BF16)

    for c in range(nblk):
        @pl.when(s == 0)
        def _():
            put_dx(gout[npp - 1, c], c, 0)

        @pl.when(s > 0)
        def _():
            hop_wait(npp - 1, c)
            put_dx(gin[npp - 1, c], c, 0)

    scale = 1.0 / ndp

    def all_of(ref, sem):
        return pltpu.make_async_copy(ref, ref, sem)

    def r2_sum(i, own):
        for k in range(1, ndp):
            own = own + recv2[slot_of[k], i].astype(F32)
        rows = pl.ds(pl.multiple_of((i // across) * rc, rc), rc)
        g2[rows, cols2(i)] = own * scale

    def r2_wait(i):
        with jax.named_scope('r2wait'):
            all_of(recv2.at[0:2, i], recv2_sem.at[i]).wait()
            all_of(recv2.at[2, i], far_recv.at[i]).wait()

    r2_wait(0)
    r2_sum(0, first[0].astype(F32))

    for u, k, b in units:
        all_of(relay_at(k, b), unit_recv.at[u]).wait()
    all_of(recv2.at[0, 1], recv2_sem.at[1]).wait()
    r2_sum(1, w2v[rows2(1, 0), cols2(1)].astype(F32))

    def r2_step(i, _):
        r2_wait(i)
        r2_sum(i, w2v[rows2(i, 0), cols2(i)].astype(F32))
        return 0

    lax.fori_loop(2, plain, r2_step, 0)

    for n in reversed(range(len(early))):
        i = early[n][0]

        @pl.when(early_on(n))
        def _():
            early_copy('acc', n, 0).wait()
            for hh in range(2):
                if hh == 0:
                    if n == 0:
                        early_copy('act', n, hh).wait()
                    early_copy('g', n, hh).wait()
                else:
                    @pl.when(s < npp - 2)
                    def _():
                        if n == 0:
                            early_copy('act', n, hh).wait()
                        early_copy('g', n, hh).wait()
            recv2[slot_of[2], i] = (early_acc[n] + dot(early_act[...], early_g[n], NT)).astype(BF16)

        @pl.when(jnp.logical_not(early_on(n)))
        def _():
            far_copy(n).wait()
        with jax.named_scope('r2wait'):
            all_of(recv2.at[0:2, i], recv2_sem.at[i]).wait()
        r2_sum(i, w2v[rows2(i, 0), cols2(i)].astype(F32))

    def r1_step(i, _):
        with jax.named_scope('r1wait'):
            all_of(recv1.at[i], recv1_sem.at[i]).wait()
        with jax.named_scope('r1sum'):
            tot = w1v[rows1(i, 0), cols1(i)].astype(F32)
            for k in range(1, ndp):
                tot = tot + recv1[i, k - 1].astype(F32)
            g1[pl.ds(pl.multiple_of((i % halves) * rc1, rc1), rc1), cols1(i)] = tot * scale
        return 0

    lax.fori_loop(0, nchunk, r1_step, 0)

    with jax.named_scope('tail'):
        all_of(recv1, send1.at[0]).wait()
        all_of(recv2.at[0:2], send2.at[0]).wait()
        all_of(recv2.at[2, 0:plain], send2.at[1]).wait()
        for u, k, b in units:
            @pl.when(is_shed(u, npp - 1 - s))
            def _():
                relay_copy(u, k, b).wait_send()
        for t in range(npp - 1):
            @pl.when(t < npp - s)
            def _():
                all_of(gout.at[t], hop_send.at[t]).wait()


def put(g1, g2, dx, o1, o2, o3, sems):
    pieces = 4
    copies = []
    for n, (src, dst) in enumerate(((g1, o1), (g2, o2))):
        size = src.shape[0] // pieces
        for i in range(pieces):
            rows = pl.ds(i * size, size)
            copies.append(pltpu.make_async_copy(src.at[rows, :], dst.at[rows, :], sems.at[n * pieces + i]))
    copies.append(pltpu.make_async_copy(dx, o3, sems.at[2 * pieces]))
    for copy in copies:
        copy.start()
    for copy in copies:
        copy.wait()


def solution(mesh):
    npp = mesh.shape['pp']
    ndp = mesh.shape['dp']

    def body(dy, xs, hs, w1, w2, acc1, acc2):
        tok = dy.shape[1]
        dm, ff = w1.shape[2:]
        ntok = npp * tok
        nchunk = 8
        blk = 256
        nblk = dm // blk
        q1, q2 = dm // ndp, ff // ndp
        rc1, cc1 = q1 // 2, ff // (nchunk // 2)
        rc, cc = q2 // 2, dm // (nchunk // 2)
        dma = pltpu.SemaphoreType.DMA
        any_spec = pl.BlockSpec(memory_space=pl.ANY)
        vmem = pl.BlockSpec(memory_space=pltpu.VMEM)
        shapes = ((q1, ff), F32), ((q2, dm), F32), ((tok, dm), BF16)
        outs = pl.pallas_call(
            functools.partial(kernel, npp, ndp, tok, nchunk),
            out_shape=tuple(pltpu.VMEM(shape, dtype) for shape, dtype in shapes),
            in_specs=[any_spec] * 7,
            out_specs=(vmem,) * 3,
            scratch_shapes=[
                pltpu.VMEM((dm, ff), BF16), pltpu.VMEM((ff, dm), BF16),
                pltpu.VMEM((nchunk, ndp - 1, rc1, cc1), BF16), pltpu.VMEM((ndp - 1, nchunk, rc, cc), BF16),
                pltpu.VMEM((ntok, ff), BF16), pltpu.VMEM((ntok, dm), BF16),
                pltpu.VMEM((ff, ntok), BF16), pltpu.VMEM((ff, ntok), F32), pltpu.VMEM((ff, ntok), BF16),
                pltpu.VMEM((dm, ntok), BF16), pltpu.VMEM((dm, ntok), BF16), pltpu.VMEM((ff, 2 * tok), F32),
                pltpu.VMEM((ndp, rc, cc), BF16),
                pltpu.VMEM((npp, nblk, blk // 2, 2 * tok), BF16), pltpu.VMEM((npp, nblk, blk // 2, 2 * tok), BF16),
                pltpu.VMEM((2, rc, cc), BF16), pltpu.VMEM((blk, blk), BF16),
                pltpu.VMEM((2, ndp, rc1, cc1), F32), pltpu.VMEM((ndp, rc, cc), F32),
                pltpu.VMEM((len(EARLY), rc, cc), F32), pltpu.VMEM((rc, ntok), BF16), pltpu.VMEM((len(EARLY), cc, ntok), BF16),
                pltpu.VMEM((tok, dm), BF16),
                dma((1,)), dma((npp,)), dma((npp,)), dma((8,)), dma((nblk,)), dma((2,)), dma((3,)),
                dma((npp - 1,)), dma((npp, nblk)),
                dma((1,)), dma((nchunk,)), dma((4,)), dma((nchunk,)), dma((nchunk,)), dma((8,)), dma((8,)), dma((8,)),
                dma((8,)), dma((8,)),
            ],
            compiler_params=pltpu.CompilerParams(
                collective_id=0, has_side_effects=True, vmem_limit_bytes=VMEM_LIMIT),
        )(dy[0], xs.reshape(ntok, dm), hs.reshape(ntok, ff), w1[0, 0], w2[0, 0], acc1[0, 0, 0], acc2[0, 0, 0])
        r1, r2, dx = pl.pallas_call(
            put,
            out_shape=tuple(jax.ShapeDtypeStruct(shape, dtype) for shape, dtype in shapes),
            in_specs=[any_spec] * 3,
            out_specs=(any_spec,) * 3,
            scratch_shapes=[dma((9,))],
            compiler_params=pltpu.CompilerParams(vmem_limit_bytes=1024 * 1024),
        )(*outs)
        return r1[None, None], r2[None, None], dx[None]

    spec_row = P(('grp', 'pp'), 'dp', None)
    spec_saved = P(('grp', 'pp'), None, None, 'dp', None)
    spec_w = P(('grp', 'pp'), None, None, None)
    spec_acc = P(('grp', 'pp'), 'dp', None, None, None)
    spec_g = P(('grp', 'pp'), None, 'dp', None)
    return jax.shard_map(body, mesh=mesh, in_specs=(spec_row, spec_saved, spec_saved, spec_w, spec_w, spec_acc, spec_acc), out_specs=(spec_g, spec_g, spec_row), check_vma=False)
```

```python
import functools

import jax
import jax.numpy as jnp
from jax import lax
from jax.experimental import pallas as pl
from jax.experimental.pallas import tpu as pltpu
from jax.sharding import PartitionSpec as P

MESH = pl.DeviceIdType.MESH
EARLY = (3,)
VMEM_LIMIT = 53 * 1024 * 1024
NN = (((1,), (0,)), ((), ()))
NT = (((1,), (1,)), ((), ()))
SQRT_2_OVER_PI = 0.7978845608028654
BF16 = jnp.bfloat16
F32 = jnp.float32


def dot(a, b, dims):
    return lax.dot_general(a, b, dims, preferred_element_type=F32)


def kernel(npp, ndp, tok, nchunk, dy, xs, hs, w1, w2, acc1, acc2, g1, g2, dx,
           w1v, w2v, recv1, recv2, hv, xv, act, slope, dht, xt, gt, uacc, first, gin, gout, relay, ident,
           stage1, stage2, early_acc, early_act, early_g, dyv,
           ld_sem, h_sem, x_sem, w2_sem, w1_sem, st1_sem, st2_sem, hop_send, hop_recv,
           send1, recv1_sem, send2, recv2_sem, far_recv, unit_recv, relay_send, relay_recv,
           early_send, early_recv):
    s = lax.axis_index('pp')
    p = lax.axis_index('dp')
    dm, ff = w1v.shape
    blk = ident.shape[0]
    half = 2 * tok
    hb = blk // 2
    nw2 = 8
    w2rows = ff // nw2
    nblk = dm // blk
    q1 = dm // ndp
    q2 = ff // ndp
    rc1, cc1 = stage1.shape[2:]
    rc, cc = first.shape[1:]
    halves = q1 // rc1
    across = dm // cc
    mrows = 1024
    shed = (6, 2)
    early = tuple(zip((nchunk - 1, nchunk - 2), EARLY))

    far = (p + 2) % ndp
    peer = (p, p + 1 - 2 * (p % 2), far, far + 1 - 2 * (far % 2))

    far_k = (2, 3)
    order = far_k + (1, 0)

    def w2_copy(i):
        rows = pl.ds(i * w2rows, w2rows)
        return pltpu.make_async_copy(w2.at[rows, :], w2v.at[rows, :], w2_sem.at[i * 2 // nw2])

    def w1_copy(i):
        rows = pl.ds(i * blk, blk)
        return pltpu.make_async_copy(w1.at[rows, :], w1v.at[rows, :], w1_sem.at[i])

    def rows1(i, k):
        return pl.ds(pl.multiple_of(peer[k] * q1 + (i % halves) * rc1, rc1), rc1)

    def cols1(i):
        return pl.ds(pl.multiple_of((i // halves) * cc1, cc1), cc1)

    def rows2(i, k):
        return pl.ds(pl.multiple_of(peer[k] * q2 + (i // across) * rc, rc), rc)

    def cols2(i):
        return pl.ds(pl.multiple_of((i % across) * cc, cc), cc)

    def acc1_copy(i, k):
        return pltpu.make_async_copy(acc1.at[rows1(i, k), cols1(i)], stage1.at[i % 2, k], st1_sem.at[i % 2])

    def acc1_wait(i):
        pltpu.make_async_copy(stage1.at[i % 2], stage1.at[i % 2], st1_sem.at[i % 2]).wait()

    def slot2(i, k, n=1):
        return pl.ds(pl.multiple_of(((i % 2) * ndp + k) * rc, rc), n * rc)

    def acc2_copy(i, k):
        return pltpu.make_async_copy(acc2.at[rows2(i, k), cols2(i)], slope.at[slot2(i, k), :], st2_sem.at[i % 2])

    def acc2_wait(i):
        span = slope.at[slot2(i, 0, ndp), :]
        pltpu.make_async_copy(span, span, st2_sem.at[i % 2]).wait()

    def first_copy(k):
        return pltpu.make_async_copy(acc2.at[rows2(0, k), cols2(0)], stage2.at[k], st2_sem.at[2])

    def h_copy(t):
        rows = pl.ds((npp - 1 - s - t) * tok, tok)
        return pltpu.make_async_copy(hs.at[rows, :], hv.at[pl.ds(t * tok, tok), :], h_sem.at[t])

    def x_copy(t):
        rows = pl.ds((npp - 1 - s - t) * tok, tok)
        return pltpu.make_async_copy(xs.at[rows, :], xv.at[pl.ds(t * tok, tok), :], x_sem.at[t])

    dy_copy = pltpu.make_async_copy(dy, dyv, ld_sem.at[0])

    def used(t, start):
        @pl.when(t < npp - s)
        def _():
            start(t)

    for t in range(2):
        used(t, lambda t: h_copy(t).start())
    dy_copy.start()
    for i in range(1):
        w2_copy(i).start()

    barrier = pltpu.get_barrier_semaphore()
    for k in range(1, ndp):
        pl.semaphore_signal(barrier, inc=1, device_id={'dp': peer[k]}, device_id_type=MESH)
    for k in range(1, npp):
        pl.semaphore_signal(barrier, inc=1, device_id={'pp': (s + k) % npp}, device_id_type=MESH)

    for k in far_k:
        pl.semaphore_signal(barrier, inc=1, device_id={'pp': npp - 1 - s, 'dp': peer[k]}, device_id_type=MESH)

    rid = lax.broadcasted_iota(jnp.int32, (blk, blk), 0)
    cid = lax.broadcasted_iota(jnp.int32, (blk, blk), 1)
    ident[...] = jnp.where(rid == cid, 1.0, 0.0).astype(BF16)
    low = lax.broadcasted_iota(jnp.int32, (hb, half), 1) < tok

    def h_wait(t):
        @pl.when(t < npp - s)
        def _():
            h_copy(t).wait()

        @pl.when(t >= npp - s)
        def _():
            hv[t * tok:(t + 1) * tok, :] = jnp.zeros((tok, ff), BF16)

    def gelu_block(i, lanes):
        rows = slice(i * blk, (i + 1) * blk) if isinstance(i, int) else pl.ds(pl.multiple_of(i * blk, blk), blk)
        h = dot(ident[...], hv[lanes, rows], NT)
        h2 = h * h
        t = jnp.tanh(h * (SQRT_2_OVER_PI + (SQRT_2_OVER_PI * 0.044715) * h2))
        cdf = 0.5 + 0.5 * t
        a = h * cdf
        act[rows, lanes] = a.astype(BF16)
        slope[rows, lanes] = cdf + (a * (1.0 - cdf)) * (2.0 * SQRT_2_OVER_PI + (6.0 * SQRT_2_OVER_PI * 0.044715) * h2)

    def gelu(hh, start, stop):
        def step(i, _):
            gelu_block(i, slice(hh * half, (hh + 1) * half))
            return 0

        with jax.named_scope('gelu'):
            lax.fori_loop(start, stop, step, 0, unroll=4)

    gt[...] = jnp.zeros_like(gt)

    @pl.when(s >= npp - 2)
    def _():
        act[:, half:] = jnp.zeros((ff, half), BF16)
        dht[:, half:] = jnp.zeros((ff, half), BF16)
        early_act[:, half:] = jnp.zeros((rc, half), BF16)
        for n in range(len(early)):
            early_g[n, :, half:] = jnp.zeros((cc, half), BF16)

    for i in range(1, nw2):
        w2_copy(i).start()
    with jax.named_scope('hwait'):
        for t in range(2):
            h_wait(t)
        dy_copy.wait()
    for c in range(nblk):
        gt[c * blk:(c + 1) * blk, 0:tok] = dot(ident[...], dyv[:, c * blk:(c + 1) * blk], NT).astype(BF16)

    at0 = 1 - jnp.minimum(s, 1)

    def hop_copy(t, c):
        slot = t + (npp - 1 - t) * at0
        return pltpu.make_async_remote_copy(
            src_ref=gout.at[t, c], dst_ref=gin.at[slot, c], send_sem=hop_send.at[t], recv_sem=hop_recv.at[slot, c],
            device_id={'pp': (s - 1) * (1 - at0) + (npp - 1 - t) * at0}, device_id_type=MESH)

    def hop_wait(slot, c):
        pltpu.make_async_remote_copy(
            src_ref=gin.at[slot, c], dst_ref=gin.at[slot, c], send_sem=hop_send.at[0], recv_sem=hop_recv.at[slot, c],
            device_id={'pp': s}, device_id_type=MESH).wait_recv()

    slot_of = {1: 0, 3: 1, 2: 2}

    def sems2(i, k):
        return dict(send_sem=send2.at[1 if k == 2 else 0], recv_sem=far_recv.at[i] if k == 2 else recv2_sem.at[i],
                    device_id={'dp': peer[k]}, device_id_type=MESH)

    def send_first(k):
        return pltpu.make_async_remote_copy(src_ref=first.at[k], dst_ref=recv2.at[slot_of[k], 0], **sems2(0, k))

    hl = (slice(0, half), slice(half, 2 * half))

    def early_on(n):
        return s < early[n][1]

    def early_copy(what, n, hh, cond_start=True):
        i = early[n][0]
        if what == 'acc':
            src, dst, q = acc2.at[rows2(i, 2), cols2(i)], early_acc.at[n], n
        elif what == 'act':
            src, dst, q = act.at[rows2(i, 2), hl[hh]], early_act.at[:, hl[hh]], 2 + hh
        else:
            src, dst, q = gt.at[cols2(i), hl[hh]], early_g.at[n, :, hl[hh]], 4 + 2 * n + hh
        return pltpu.make_async_remote_copy(
            src_ref=src, dst_ref=dst, send_sem=early_send.at[q], recv_sem=early_recv.at[q],
            device_id={'dp': peer[2]}, device_id_type=MESH)

    def early_start():
        for n in range(len(early)):
            @pl.when(early_on(n))
            def _():
                early_copy('acc', n, 0).start()

    def early_gt(hh, cond=None):
        for n in range(len(early)):
            @pl.when(early_on(n) if cond is None else early_on(n) & cond)
            def _():
                early_copy('g', n, hh).start()


    def first_chunk():
        with jax.named_scope('first'):
            pltpu.make_async_copy(stage2, stage2, st2_sem.at[2]).wait()
            for k in order:
                first[k] = (stage2[k] + dot(act[rows2(0, k), :], gt[0:cc, :], NT)).astype(BF16)
                if k == order[1]:
                    send_first(order[0]).start()
                    send_first(order[1]).start()
            send_first(order[2]).start()

    def unpack(packed, c, t):
        lanes = slice((t // 2) * half, (t // 2 + 1) * half)
        v = packed.astype(F32)
        r = pltpu.roll(v, tok, 1)
        for b, (lo, hi) in enumerate(((v, r), (r, v))):
            rows = slice(c * blk + b * hb, c * blk + (b + 1) * hb)
            if t % 2 == 0:
                new = jnp.where(low, lo, 0.0)
            else:
                new = jnp.where(low, gt[rows, lanes].astype(F32), hi)
            gt[rows, lanes] = new.astype(BF16)

    for t in range(npp):
        lanes = slice((t // 2) * half, (t // 2 + 1) * half)

        @pl.when(t < npp - s)
        def _(t=t, lanes=lanes):
            if t == 0:
                gelu(0, 0, ff // blk // 2)
                with jax.named_scope('barrier'):
                    pl.semaphore_wait(barrier, ndp - 1 + npp - 1 + len(far_k))
                early_start()
                with jax.named_scope('u0'):
                    for part in range(2):
                        w2half = w2v.at[pl.ds(part * (ff // 2), ff // 2), :]
                        pltpu.make_async_copy(w2half, w2half, w2_sem.at[part]).wait()
                        if part == 0:
                            @pl.when(s == npp - 1)
                            def _():
                                for k in range(ndp):
                                    first_copy(k).start()
                            for i in range(nblk):
                                w1_copy(i).start()
                        for c in range(nblk):
                            krows = slice(c * blk, (c + 1) * blk)
                            for i in range(ff // mrows // 2):
                                rows = slice(part * (ff // 2) + i * mrows, part * (ff // 2) + (i + 1) * mrows)
                                u = dot(w2v[rows, krows], gt[krows, lanes], NN)
                                if c > 0:
                                    u = uacc[rows, :] + u
                                if c < nblk - 1:
                                    uacc[rows, :] = u
                                else:
                                    dht[rows, lanes] = (slope[rows, lanes] * u).astype(BF16)
                                if part == 0:
                                    gelu_block(ff // blk // 2 + c * 2 + i, lanes)

                @pl.when(early_on(0))
                def _():
                    early_copy('act', 0, 0).start()
                for t2 in range(2, npp):
                    used(t2, lambda t2: h_copy(t2).start())
                for t2 in range(npp):
                    used(t2, lambda t2: x_copy(t2).start())
            else:
                groups = ((0,), (1,), (2,), (3,))
                for group in groups:
                    for c in group:
                        with jax.named_scope('gwait'):
                            hop_wait(t - 1, c)
                        unpack(gin[t - 1, c], c, t)
                    if group == groups[-1]:
                        if t == npp - 1:
                            first_chunk()
                            early_gt(1)
                        elif t == npp - 2:
                            early_gt(1, s == 1)
                        elif t == 1:
                            early_gt(0)
                    krows = slice(group[0] * blk, (group[-1] + 1) * blk)

                    with jax.named_scope('u'):
                        for i in range(ff // mrows):
                            rows = slice(i * mrows, (i + 1) * mrows)
                            u = dot(w2v[rows, krows], gt[krows, lanes], NN)
                            if group != groups[0]:
                                u = uacc[rows, :] + u
                            if group != groups[-1]:
                                uacc[rows, :] = u
                            else:
                                dht[rows, lanes] = (slope[rows, lanes] * u).astype(BF16)

            def gx_dot(c, part):
                rows = slice(c * blk, (c + 1) * blk)
                k = slice(part * (ff // 2), (part + 1) * (ff // 2))
                return dot(w1v[rows, k], dht[k, lanes], NN)

            def gx_put(c, z):
                top, bot = z[:hb], z[hb:]
                if t % 2 == 0:
                    z = jnp.where(low, top, pltpu.roll(bot, tok, 1))
                else:
                    z = jnp.where(low, pltpu.roll(top, tok, 1), bot)
                gout[t, c] = z.astype(BF16)

                if t < npp - 1:
                    hop_copy(t, c).start()

            with jax.named_scope('gx'):
                last = None
                for c in range(nblk):
                    if t == 0 and c % 2 == 0:
                        w1_copy(c).wait()
                        w1_copy(c + 1).wait()
                    if t == 0 and c == 0:
                        @pl.when(s < npp - 1)
                        def _():
                            for k in range(ndp):
                                first_copy(k).start()
                        for i in range(2):
                            for k in range(ndp):
                                acc1_copy(i, k).start()
                    if t == 0 and c == 2:
                        gx_put(1, last)

                        @pl.when(s == npp - 1)
                        def _():
                            first_chunk()
                    if c > 0 and not (t == 0 and c == 2):
                        gx_put(c - 1, last)
                    z = gt[c * blk:(c + 1) * blk, lanes].astype(F32) + gx_dot(c, 0)
                    last = z + gx_dot(c, 1)
                gx_put(nblk - 1, last)

        if t == 0:
            @pl.when(s < npp - 2)
            def _():
                for t in range(2, npp):
                    h_wait(t)
                gelu(1, 0, ff // blk)

                @pl.when(early_on(0))
                def _():
                    early_copy('act', 0, 1).start()

    for i in range(1, 3):
        for k in range(ndp):
            acc2_copy(i, k).start()

    @pl.when((s > 0) & (s < npp - 1))
    def _():
        first_chunk()

    for t in range(npp):
        @pl.when(t < npp - s)
        def _():
            x_copy(t).wait()

        @pl.when(t >= npp - s)
        def _():
            xv[t * tok:(t + 1) * tok, :] = jnp.zeros((tok, dm), BF16)
    for c in range(nblk):
        rows = pl.ds(c * blk, blk)
        xt[rows, :] = dot(ident[...], xv[:, rows], NT).astype(BF16)

    def send2_copy(i, k):
        return pltpu.make_async_remote_copy(
            src_ref=w2v.at[rows2(i, k), cols2(i)], dst_ref=recv2.at[slot_of[k], i], **sems2(i, k))

    def send1_copy(i, k):
        return pltpu.make_async_remote_copy(
            src_ref=w1v.at[rows1(i, k), cols1(i)], dst_ref=recv1.at[i, k - 1],
            send_sem=send1.at[0], recv_sem=recv1_sem.at[i], device_id={'dp': peer[k]}, device_id_type=MESH)

    pieces = ((0, rc // 4), (rc // 4, rc // 8), (3 * rc // 8, rc // 8), (rc // 2, rc // 2))
    units = tuple((u, far_k[u // 4], pieces[u % 4]) for u in range(8))

    def is_shed(u, stage):
        cond = jnp.bool_(False)
        for n, count in enumerate(shed):
            if u < count:
                cond = cond | (stage == n)
        return cond

    def unit_dst(k, b):
        return recv2.at[slot_of[k], 1, pl.ds(*b), :]

    def unit_src(k, b):
        return w2v.at[pl.ds(pl.multiple_of(peer[k] * q2 + b[0], rc // 8), b[1]), cols2(1)]

    def relay_at(k, b):
        return relay.at[far_k.index(k), pl.ds(*b), :]

    def unit_copy(u, k, b):
        return pltpu.make_async_remote_copy(
            src_ref=unit_src(k, b), dst_ref=unit_dst(k, b), send_sem=send2.at[1 if k == 2 else 0], recv_sem=unit_recv.at[u],
            device_id={'dp': peer[k]}, device_id_type=MESH)

    def shed_copy(u, k, b):
        return pltpu.make_async_remote_copy(
            src_ref=unit_src(k, b), dst_ref=relay_at(k, b), send_sem=send2.at[1 if k == 2 else 0], recv_sem=relay_recv.at[u],
            device_id={'pp': npp - 1 - s, 'dp': peer[k]}, device_id_type=MESH)

    def relay_copy(u, k, b):
        return pltpu.make_async_remote_copy(
            src_ref=relay_at(k, b), dst_ref=unit_dst(k, b), send_sem=relay_send.at[u], recv_sem=unit_recv.at[u],
            device_id={'pp': npp - 1 - s}, device_id_type=MESH)

    def send_unit(u, k, b):
        cond = is_shed(u, s)

        @pl.when(cond)
        def _():
            shed_copy(u, k, b).start()

        @pl.when(jnp.logical_not(cond))
        def _():
            unit_copy(u, k, b).start()

    def a2_add(i):
        acc2_wait(i)
        for k in order:
            w2v[rows2(i, k), cols2(i)] = (
                slope[slot2(i, k), :] + dot(act[rows2(i, k), :], gt[cols2(i), :], NT)).astype(BF16)

    def a2_next(i):
        @pl.when(i + 2 < nchunk)
        def _():
            for k in range(ndp):
                acc2_copy(i + 2, k).start()

    plain = nchunk - len(early)

    def a2_step(i, _):
        a2_add(i)
        for k in order[:-1]:
            send2_copy(i, k).start()
        a2_next(i)
        return 0

    def far_copy(n):
        i = early[n][0]
        return pltpu.make_async_remote_copy(
            src_ref=w2v.at[rows2(i, 2), cols2(i)], dst_ref=recv2.at[slot_of[2], i],
            send_sem=send2.at[2 + n], recv_sem=far_recv.at[i], device_id={'dp': peer[2]}, device_id_type=MESH)

    with jax.named_scope('a2'):
        a2_add(1)
        for unit in units:
            send_unit(*unit)
        send2_copy(1, 1).start()
        a2_next(jnp.int32(1))
        lax.fori_loop(2, plain, a2_step, 0)
        for n in reversed(range(len(early))):
            i = early[n][0]
            a2_add(i)

            @pl.when(jnp.logical_not(early_on(n)))
            def _():
                far_copy(n).start()
            for k in (3, 1):
                send2_copy(i, k).start()

    with jax.named_scope('relay'):
        for u, k, b in units:
            @pl.when(is_shed(u, npp - 1 - s))
            def _():
                pltpu.make_async_remote_copy(
                    src_ref=relay_at(k, b), dst_ref=relay_at(k, b), send_sem=relay_send.at[u], recv_sem=relay_recv.at[u],
                    device_id={'pp': npp - 1 - s}, device_id_type=MESH).wait_recv()
                relay_copy(u, k, b).start()

    def a1_step(i, _):
        acc1_wait(i)
        for k in order:
            w1v[rows1(i, k), cols1(i)] = (
                stage1[i % 2, k] + dot(xt[rows1(i, k), :], dht[cols1(i), :], NT)).astype(BF16)
        for k in order[:-1]:
            send1_copy(i, k).start()

        @pl.when(i + 2 < nchunk)
        def _():
            for k in range(ndp):
                acc1_copy(i + 2, k).start()
        return 0

    with jax.named_scope('a1'):
        lax.fori_loop(0, nchunk, a1_step, 0)

    def put_dx(packed, c, e):
        v = packed.astype(F32)
        r = pltpu.roll(v, tok, 1)
        col = jnp.concatenate([v, r], axis=0).astype(BF16)
        dx[:, c * blk:(c + 1) * blk] = dot(ident[:tok, :half], col, NT).astype(BF16)

    for c in range(nblk):
        @pl.when(s == 0)
        def _():
            put_dx(gout[npp - 1, c], c, 0)

        @pl.when(s > 0)
        def _():
            hop_wait(npp - 1, c)
            put_dx(gin[npp - 1, c], c, 0)

    scale = 1.0 / ndp

    def all_of(ref, sem):
        return pltpu.make_async_copy(ref, ref, sem)

    def r2_sum(i, own):
        for k in range(1, ndp):
            own = own + recv2[slot_of[k], i].astype(F32)
        rows = pl.ds(pl.multiple_of((i // across) * rc, rc), rc)
        g2[rows, cols2(i)] = own * scale

    def r2_wait(i):
        with jax.named_scope('r2wait'):
            all_of(recv2.at[0:2, i], recv2_sem.at[i]).wait()
            all_of(recv2.at[2, i], far_recv.at[i]).wait()

    r2_wait(0)
    r2_sum(0, first[0].astype(F32))

    for u, k, b in units:
        all_of(relay_at(k, b), unit_recv.at[u]).wait()
    all_of(recv2.at[0, 1], recv2_sem.at[1]).wait()
    r2_sum(1, w2v[rows2(1, 0), cols2(1)].astype(F32))

    def r2_step(i, _):
        r2_wait(i)
        r2_sum(i, w2v[rows2(i, 0), cols2(i)].astype(F32))
        return 0

    lax.fori_loop(2, plain, r2_step, 0)

    for n in reversed(range(len(early))):
        i = early[n][0]

        @pl.when(early_on(n))
        def _():
            early_copy('acc', n, 0).wait()
            for hh in range(2):
                if hh == 0:
                    if n == 0:
                        early_copy('act', n, hh).wait()
                    early_copy('g', n, hh).wait()
                else:
                    @pl.when(s < npp - 2)
                    def _():
                        if n == 0:
                            early_copy('act', n, hh).wait()
                        early_copy('g', n, hh).wait()
            recv2[slot_of[2], i] = (early_acc[n] + dot(early_act[...], early_g[n], NT)).astype(BF16)

        @pl.when(jnp.logical_not(early_on(n)))
        def _():
            far_copy(n).wait()
        with jax.named_scope('r2wait'):
            all_of(recv2.at[0:2, i], recv2_sem.at[i]).wait()
        r2_sum(i, w2v[rows2(i, 0), cols2(i)].astype(F32))

    def r1_step(i, _):
        with jax.named_scope('r1wait'):
            all_of(recv1.at[i], recv1_sem.at[i]).wait()
        with jax.named_scope('r1sum'):
            tot = w1v[rows1(i, 0), cols1(i)].astype(F32)
            for k in range(1, ndp):
                tot = tot + recv1[i, k - 1].astype(F32)
            g1[pl.ds(pl.multiple_of((i % halves) * rc1, rc1), rc1), cols1(i)] = tot * scale
        return 0

    lax.fori_loop(0, nchunk, r1_step, 0)

    with jax.named_scope('tail'):
        all_of(recv1, send1.at[0]).wait()
        all_of(recv2.at[0:2], send2.at[0]).wait()
        all_of(recv2.at[2, 0:plain], send2.at[1]).wait()
        for u, k, b in units:
            @pl.when(is_shed(u, npp - 1 - s))
            def _():
                relay_copy(u, k, b).wait_send()
        for t in range(npp - 1):
            @pl.when(t < npp - s)
            def _():
                all_of(gout.at[t], hop_send.at[t]).wait()


def put(g1, g2, dx, o1, o2, o3, sems):
    pieces = 4
    copies = []
    for n, (src, dst) in enumerate(((g1, o1), (g2, o2))):
        size = src.shape[0] // pieces
        for i in range(pieces):
            rows = pl.ds(i * size, size)
            copies.append(pltpu.make_async_copy(src.at[rows, :], dst.at[rows, :], sems.at[n * pieces + i]))
    copies.append(pltpu.make_async_copy(dx, o3, sems.at[2 * pieces]))
    for copy in copies:
        copy.start()
    for copy in copies:
        copy.wait()


def solution(mesh):
    npp = mesh.shape['pp']
    ndp = mesh.shape['dp']

    def body(dy, xs, hs, w1, w2, acc1, acc2):
        tok = dy.shape[1]
        dm, ff = w1.shape[2:]
        ntok = npp * tok
        nchunk = 8
        blk = 256
        nblk = dm // blk
        q1, q2 = dm // ndp, ff // ndp
        rc1, cc1 = q1 // 2, ff // (nchunk // 2)
        rc, cc = q2 // 2, dm // (nchunk // 2)
        dma = pltpu.SemaphoreType.DMA
        any_spec = pl.BlockSpec(memory_space=pl.ANY)
        vmem = pl.BlockSpec(memory_space=pltpu.VMEM)
        shapes = ((q1, ff), F32), ((q2, dm), F32), ((tok, dm), BF16)
        outs = pl.pallas_call(
            functools.partial(kernel, npp, ndp, tok, nchunk),
            out_shape=tuple(pltpu.VMEM(shape, dtype) for shape, dtype in shapes),
            in_specs=[any_spec] * 7,
            out_specs=(vmem,) * 3,
            scratch_shapes=[
                pltpu.VMEM((dm, ff), BF16), pltpu.VMEM((ff, dm), BF16),
                pltpu.VMEM((nchunk, ndp - 1, rc1, cc1), BF16), pltpu.VMEM((ndp - 1, nchunk, rc, cc), BF16),
                pltpu.VMEM((ntok, ff), BF16), pltpu.VMEM((ntok, dm), BF16),
                pltpu.VMEM((ff, ntok), BF16), pltpu.VMEM((ff, ntok), F32), pltpu.VMEM((ff, ntok), BF16),
                pltpu.VMEM((dm, ntok), BF16), pltpu.VMEM((dm, ntok), BF16), pltpu.VMEM((ff, 2 * tok), F32),
                pltpu.VMEM((ndp, rc, cc), BF16),
                pltpu.VMEM((npp, nblk, blk // 2, 2 * tok), BF16), pltpu.VMEM((npp, nblk, blk // 2, 2 * tok), BF16),
                pltpu.VMEM((2, rc, cc), BF16), pltpu.VMEM((blk, blk), BF16),
                pltpu.VMEM((2, ndp, rc1, cc1), F32), pltpu.VMEM((ndp, rc, cc), F32),
                pltpu.VMEM((len(EARLY), rc, cc), F32), pltpu.VMEM((rc, ntok), BF16), pltpu.VMEM((len(EARLY), cc, ntok), BF16),
                pltpu.VMEM((tok, dm), BF16),
                dma((1,)), dma((npp,)), dma((npp,)), dma((2,)), dma((nblk,)), dma((2,)), dma((3,)),
                dma((npp - 1,)), dma((npp, nblk)),
                dma((1,)), dma((nchunk,)), dma((4,)), dma((nchunk,)), dma((nchunk,)), dma((8,)), dma((8,)), dma((8,)),
                dma((8,)), dma((8,)),
            ],
            compiler_params=pltpu.CompilerParams(
                collective_id=0, has_side_effects=True, vmem_limit_bytes=VMEM_LIMIT),
        )(dy[0], xs.reshape(ntok, dm), hs.reshape(ntok, ff), w1[0, 0], w2[0, 0], acc1[0, 0, 0], acc2[0, 0, 0])
        r1, r2, dx = pl.pallas_call(
            put,
            out_shape=tuple(jax.ShapeDtypeStruct(shape, dtype) for shape, dtype in shapes),
            in_specs=[any_spec] * 3,
            out_specs=(any_spec,) * 3,
            scratch_shapes=[dma((9,))],
            compiler_params=pltpu.CompilerParams(vmem_limit_bytes=1024 * 1024),
        )(*outs)
        return r1[None, None], r2[None, None], dx[None]

    spec_row = P(('grp', 'pp'), 'dp', None)
    spec_saved = P(('grp', 'pp'), None, None, 'dp', None)
    spec_w = P(('grp', 'pp'), None, None, None)
    spec_acc = P(('grp', 'pp'), 'dp', None, None, None)
    spec_g = P(('grp', 'pp'), None, 'dp', None)
    return jax.shard_map(body, mesh=mesh, in_specs=(spec_row, spec_saved, spec_saved, spec_w, spec_w, spec_acc, spec_acc), out_specs=(spec_g, spec_g, spec_row), check_vma=False)
```
